8 devices in a mesh: dp: 2 (over z, y), ep: 4 (over x, core).
Axes of the slice: x: 2, y: 2, z: 1, core: 2. Of those that a mesh axis runs over, the one named last changes fastest.
Arguments:
- tokens: bfloat16 [8192, 768], P(('dp', 'ep')), parts along dimension 0
- topk_idx: int32 [8192, 1], P(('dp', 'ep')), parts along dimension 0
- topk_w: float32 [8192, 1], P(('dp', 'ep')), parts along dimension 0
- w_up: bfloat16 [4, 5, 768, 3072], P('ep')
- w_down: bfloat16 [4, 5, 3072, 768], P('ep')
- slot_expert: int32 [4, 5], replicated
Outputs:
- output: bfloat16 [8192, 768], P(('dp', 'ep')), parts along dimension 0
There are 2 independent parts. The reference program is written for one: setup_inputs(seed, part) draws one part's arguments, and reference() takes and returns one part's arrays. A program takes and returns all parts, laid end to end along the dimension named above; an argument that names none is the same for every part.
All inputs are finite; a program needn't handle non-finite values.
Results may differ from the reference program's by a relative error of at most 0.001.
Values are sent between devices in bfloat16 or wider.
A program may use at most 1 GiB of HBM per device.

```python
import jax
import jax.numpy as jnp
from jax import lax
import numpy as np

GROUP = 4
TOK_DEV = 1024
D_MODEL = 768
D_FF = 3072
EXPERTS = 16
TOP = 1

PER_DEV = EXPERTS // GROUP
SLOTS = PER_DEV + 1
N_UNITS = GROUP * SLOTS
PAIRS_DEV = TOK_DEV * TOP
BASE_LOAD = PAIRS_DEV // N_UNITS
BLOCK = max(8, (GROUP * PAIRS_DEV) // N_UNITS)
N_BLOCKS = (GROUP * PAIRS_DEV) // BLOCK + EXPERTS


def base_table():
    dev_ids = np.arange(GROUP)
    hot_dev = (3 * (dev_ids // 3) + 3) % GROUP
    spare_exp = hot_dev * PER_DEV + PER_DEV - 1
    primary = np.arange(EXPERTS).reshape(GROUP, PER_DEV)
    return np.concatenate([primary, spare_exp[:, None]], axis=1).astype(np.int32)


def draw_table(key_tab):
    key_dev, key_col, key_lab = jax.random.split(key_tab, 3)
    relabel = jax.random.permutation(key_lab, EXPERTS).astype(jnp.int32)
    dev_perm = jax.random.permutation(key_dev, GROUP)
    col_perm = jax.random.permutation(key_col, SLOTS)
    slot_table = jnp.asarray(base_table())[dev_perm][:, col_perm]
    return relabel[slot_table], relabel


def draw_loads(key_load):
    key_perm, key_shift = jax.random.split(key_load)
    unit_order = 1 + jax.random.permutation(key_perm, N_UNITS - 1)
    shift_amt = jax.random.randint(key_shift, ((N_UNITS - 2) // 2,), 0, BASE_LOAD // 2 + 1, dtype=jnp.int32)
    spread = BASE_LOAD // 2 + 1
    unit_loads = jnp.full((N_UNITS,), BASE_LOAD, jnp.int32)
    unit_loads = unit_loads.at[0].add(spread).at[unit_order[0]].add(-spread)
    unit_loads = unit_loads.at[unit_order[1::2]].add(shift_amt).at[unit_order[2::2]].add(-shift_amt)
    return unit_loads.at[unit_order[:PAIRS_DEV - N_UNITS * BASE_LOAD]].add(1)


def draw_routing(key_src, unit_expert):
    key_load, key_tok = jax.random.split(key_src)
    counts = jax.ops.segment_sum(draw_loads(key_load), unit_expert, num_segments=EXPERTS)
    bounds = jnp.cumsum(counts)
    sorted_exp = jnp.searchsorted(bounds, jnp.arange(PAIRS_DEV, dtype=jnp.int32), side='right').astype(jnp.int32)
    routes = sorted_exp.reshape(TOP, TOK_DEV).T
    return routes[jax.random.permutation(key_tok, TOK_DEV)]


def setup_inputs(seed: int = 0, part: int = 0) -> dict:
    root_key = jax.random.key(seed)
    key_tab, key_up, key_down, key_part = jax.random.split(root_key, 4)
    slot_expert, relabel = draw_table(key_tab)
    unit_expert = relabel[jnp.asarray(base_table()).reshape(-1)]
    up_base = jax.random.normal(key_up, (EXPERTS, D_MODEL, D_FF), jnp.float32) * D_MODEL ** -0.5
    down_base = jax.random.normal(key_down, (EXPERTS, D_FF, D_MODEL), jnp.float32) * D_FF ** -0.5
    key_grp = jax.random.fold_in(key_part, part)
    key_tokens, key_gate, key_route = jax.random.split(key_grp, 3)
    tokens = jax.random.normal(key_tokens, (GROUP * TOK_DEV, D_MODEL), jnp.float32)
    topk_w = jax.random.uniform(key_gate, (GROUP * TOK_DEV, TOP), jnp.float32, 0.3, 1.0)
    src_keys = jax.random.split(key_route, GROUP)
    topk_idx = jax.vmap(draw_routing, in_axes=(0, None))(src_keys, unit_expert)
    return {'tokens': tokens.astype(jnp.bfloat16), 'topk_idx': topk_idx.reshape(GROUP * TOK_DEV, TOP), 'topk_w': topk_w, 'w_up': up_base.astype(jnp.bfloat16)[slot_expert], 'w_down': down_base.astype(jnp.bfloat16)[slot_expert], 'slot_expert': slot_expert}


def reference(tokens, topk_idx, topk_w, w_up, w_down, slot_expert):
    n_tok = tokens.shape[0]
    n_pairs = n_tok * TOP
    table_flat = slot_expert.reshape(-1)
    first_slot = jax.ops.segment_min(jnp.arange(N_UNITS, dtype=jnp.int32), table_flat, num_segments=EXPERTS)
    up_flat = w_up.reshape(N_UNITS, D_MODEL, D_FF)
    down_flat = w_down.reshape(N_UNITS, D_FF, D_MODEL)
    flat_exp = topk_idx.reshape(-1)
    flat_gate = topk_w.reshape(-1)
    pair_order = jnp.argsort(flat_exp, stable=True)
    counts = jnp.bincount(flat_exp, length=EXPERTS)
    starts = jnp.cumsum(counts) - counts
    exp_blocks = (counts + BLOCK - 1) // BLOCK
    block_end = jnp.cumsum(exp_blocks)
    block_start = block_end - exp_blocks
    lane_ids = jnp.arange(BLOCK)

    def block_step(acc_sum, block_id):
        exp_id = jnp.minimum(jnp.searchsorted(block_end, block_id, side='right'), EXPERTS - 1)
        offsets = (block_id - block_start[exp_id]) * BLOCK + lane_ids
        is_valid = (offsets < counts[exp_id]) & (block_id < block_end[EXPERTS - 1])
        pair_ids = pair_order[jnp.clip(starts[exp_id] + offsets, 0, n_pairs - 1)]
        tok_ids = pair_ids // TOP
        slot_id = first_slot[exp_id]
        pre_act = jnp.dot(tokens[tok_ids], up_flat[slot_id], preferred_element_type=jnp.float32)
        hidden = jax.nn.gelu(pre_act, approximate=True).astype(jnp.bfloat16)
        expert_out = jnp.dot(hidden, down_flat[slot_id], preferred_element_type=jnp.float32).astype(jnp.bfloat16)
        gate_vals = jnp.where(is_valid, flat_gate[pair_ids], 0.0)
        return acc_sum.at[tok_ids].add(gate_vals[:, None] * expert_out.astype(jnp.float32)), None

    acc_out, _ = lax.scan(block_step, jnp.zeros((n_tok, D_MODEL), jnp.float32), jnp.arange(N_BLOCKS))
    return acc_out.astype(jnp.bfloat16)
```

```python
import functools

import jax
import jax.numpy as jnp
from jax import lax
from jax.experimental import pallas as pl
from jax.experimental.pallas import tpu as pltpu
from jax.sharding import PartitionSpec as P

MAX_COPIES = 4
SEG = 80
N_SEG = 4
SEG_ROWS = 256
SLOT_ROWS = 4 * SEG
LOCAL_BASE = N_SEG * SEG_ROWS
LOCAL_ROWS = 1664
FF_TILE = 512
N_WBUF = 4
MESH = pl.DeviceIdType.MESH


def slot_bound(n_tok, n_top, n_dev, n_slot):
    base_load = (n_tok * n_top) // (n_dev * n_slot)
    return base_load + base_load // 2 + 1


def route_pairs(topk_idx, slot_expert, capacity):
    n_dev, n_slot = slot_expert.shape
    n_exp = n_dev * (n_slot - 1)
    n_top = topk_idx.shape[1]
    table_flat = slot_expert.reshape(-1)
    slot_ids = jnp.arange(n_dev * n_slot, dtype=jnp.int32)
    same_exp = table_flat[:, None] == table_flat[None, :]
    earlier = slot_ids[None, :] < slot_ids[:, None]
    copy_rank = jnp.sum(same_exp & earlier, axis=1, dtype=jnp.int32)
    exp_copies = jax.ops.segment_sum(jnp.ones_like(table_flat), table_flat, num_segments=n_exp)
    slot_of = jnp.zeros((n_exp, MAX_COPIES), jnp.int32).at[table_flat, copy_rank].set(slot_ids)
    flat_exp = topk_idx.reshape(-1)
    onehot = (flat_exp[:, None] == jnp.arange(n_exp, dtype=jnp.int32)[None, :]).astype(jnp.int32)
    pair_rank = jnp.sum((jnp.cumsum(onehot, axis=0) - onehot) * onehot, axis=1)
    pair_copies = exp_copies[flat_exp]
    slot_flat = slot_of[flat_exp, pair_rank % pair_copies]
    buf_row = pair_rank // pair_copies
    pair_pos = ((slot_flat % n_slot) * n_dev + slot_flat // n_slot) * capacity + buf_row
    pair_tok = jnp.arange(flat_exp.shape[0], dtype=jnp.int32) // n_top
    buf_tok = jnp.zeros((n_slot * n_dev * capacity,), jnp.int32).at[pair_pos].set(pair_tok)
    return pair_pos, buf_tok


def expert_ffn(recv_buf, up_local, down_local):
    pre_act = jnp.einsum('spcm,smf->spcf', recv_buf, up_local, preferred_element_type=jnp.float32)
    hidden = jax.nn.gelu(pre_act, approximate=True).astype(jnp.bfloat16)
    return jnp.einsum('spcf,sfm->spcm', hidden, down_local, preferred_element_type=jnp.float32).astype(jnp.bfloat16)


def general_layer(tokens, topk_idx, w_up, w_down, slot_expert):
    n_tok, d_model = tokens.shape
    n_top = topk_idx.shape[1]
    n_dev, n_slot = slot_expert.shape
    capacity = slot_bound(n_tok, n_top, n_dev, n_slot)
    pair_pos, buf_tok = route_pairs(topk_idx, slot_expert, capacity)
    send_buf = tokens[buf_tok].reshape(n_slot, n_dev, capacity, d_model)
    recv_buf = lax.all_to_all(send_buf, 'ep', 1, 1, tiled=True)
    expert_out = expert_ffn(recv_buf, w_up[0], w_down[0])
    back_buf = lax.all_to_all(expert_out, 'ep', 1, 1, tiled=True)
    return back_buf.reshape(-1, d_model)[pair_pos]


def route(idx_row, table, peers, n_exp, n_slot):
    f32 = jnp.float32
    n_tok = idx_row.shape[1]
    lanes = 128
    exp_id = lax.broadcasted_iota(jnp.int32, (n_exp, lanes), 0)
    match = [[(exp_id == table[d, s]).astype(f32) for s in range(n_slot)] for d in peers]
    copies = sum(sum(row) for row in match)
    hot = (copies == 4.0).astype(f32)
    own = sum(match[0])
    own_slot = sum(s * match[0][s] for s in range(n_slot))
    seen = jnp.zeros((n_exp, lanes), f32)
    base = [jnp.zeros((n_exp, lanes), f32) for _ in range(MAX_COPIES)]
    for r in range(len(peers)):
        passed = jnp.zeros((1, lanes), f32)
        for s in range(n_slot):
            here = match[r][s]
            local = LOCAL_BASE + SLOT_ROWS * own_slot + SEG * r
            if r == 0:
                code = local
            else:
                seg = s - passed
                code = jnp.where(own > 0, local, SEG_ROWS * seg + SEG * (r - 1))
                passed = passed + jnp.sum(here * hot, axis=0, keepdims=True)
            for c in range(MAX_COPIES):
                base[c] = jnp.where((here > 0) & (seen == c), code, base[c])
            seen = seen + here
    hot_slot = sum(s * jnp.sum(match[0][s] * hot, axis=0, keepdims=True) for s in range(n_slot))

    wide = lambda a: jnp.concatenate([a] * (n_tok // lanes), axis=1)
    onehot = (lax.broadcasted_iota(jnp.int32, (n_exp, n_tok), 0) == idx_row).astype(f32)
    step = 256
    blocks = [onehot[:, b * step:(b + 1) * step] for b in range(n_tok // step)]
    before = lax.broadcasted_iota(jnp.int32, (step, step), 0) < lax.broadcasted_iota(jnp.int32, (step, step), 1)
    local_rank = jnp.dot(jnp.concatenate(blocks, axis=0).astype(jnp.bfloat16), before.astype(f32).astype(jnp.bfloat16), preferred_element_type=f32)
    carry = jnp.zeros((n_exp, 1), f32)
    ranks = []
    for b, block in enumerate(blocks):
        ranks.append(local_rank[b * n_exp:(b + 1) * n_exp] + carry)
        carry = carry + jnp.sum(block, axis=1, keepdims=True)
    rank = jnp.concatenate(ranks, axis=1)
    n_copy = wide(copies)
    row = jnp.floor((rank + 0.5) * wide(1.0 / copies))
    which = rank - row * n_copy
    start = wide(base[3])
    for c in range(MAX_COPIES - 1):
        start = jnp.where(which == c, wide(base[c]), start)
    code = jnp.sum(onehot * (start + row), axis=0, keepdims=True)
    return code.astype(jnp.int32), hot_slot


def layer_kernel(table, tokens, idx_row, w_up, w_down, out, up_buf, down_buf, send, recv, x_buf, acc, result, back_send, back_recv, code_row, code_col, w_sem, ds_sem, dr_sem, bs_sem, br_sem):
    f32, bf16 = jnp.float32, jnp.bfloat16
    n_tok, d_model = tokens.shape
    n_slot = w_up.shape[0]
    d_ff = w_up.shape[2]
    me = lax.axis_index('ep')
    chip, core = me // 2, me % 2
    peers = [me, 2 * chip + (1 - core), 2 * (1 - chip) + core, 2 * (1 - chip) + (1 - core)]

    barrier = pltpu.get_barrier_semaphore()
    for r in (1, 2, 3):
        pl.semaphore_signal(barrier, inc=1, device_id={'ep': peers[r]}, device_id_type=MESH)

    def weight_copies(s):
        b = s % N_WBUF
        return (pltpu.make_async_copy(w_up.at[s], up_buf.at[b], w_sem.at[s, 0]),
                pltpu.make_async_copy(w_down.at[s], down_buf.at[b], w_sem.at[s, 1]))

    for s in range(N_WBUF):
        for copy in weight_copies(s):
            copy.start()

    code, hot_slot = route(idx_row[...], table, peers, 16, n_slot)
    code_row[...] = jnp.broadcast_to(code, code_row.shape)
    code_col[...] = jnp.transpose(jnp.broadcast_to(code, (128, n_tok)))
    hot_slot = hot_slot[:, :1]
    back_recv[:, 3 * SEG:, :] = jnp.zeros((N_SEG, SEG_ROWS - 3 * SEG, d_model), bf16)
    result[n_slot * SLOT_ROWS:, :] = jnp.zeros((LOCAL_ROWS - n_slot * SLOT_ROWS, d_model), bf16)

    def pick(first, rows):
        ids = lax.broadcasted_iota(jnp.int32, (rows, n_tok), 0) + first
        mask = (ids == code_row[0:1, :]).astype(f32).astype(bf16)
        return jnp.dot(mask, tokens[...], preferred_element_type=f32).astype(bf16)

    def dispatch_copy(k, r):
        rows = pl.ds((r - 1) * SEG, SEG)
        return pltpu.make_async_remote_copy(
            src_ref=send.at[k, rows], dst_ref=recv.at[k, rows],
            send_sem=ds_sem.at[k, r - 1], recv_sem=dr_sem.at[k, r - 1],
            device_id={'ep': peers[r]}, device_id_type=MESH)

    def back_copy(k, r):
        rows = pl.ds((r - 1) * SEG, SEG)
        return pltpu.make_async_remote_copy(
            src_ref=back_send.at[k, rows], dst_ref=back_recv.at[k, rows],
            send_sem=bs_sem.at[k, r - 1], recv_sem=br_sem.at[k, r - 1],
            device_id={'ep': peers[r]}, device_id_type=MESH)

    for k in range(N_SEG):
        send[k] = pick(k * SEG_ROWS, SEG_ROWS)
        if k == 0:
            pl.semaphore_wait(barrier, 3)
        for r in (2, 3, 1):
            dispatch_copy(k, r).start()

    for s in range(n_slot):
        x_buf[...] = pick(LOCAL_BASE + s * SLOT_ROWS, SLOT_ROWS)
        if s < N_SEG:
            for r in (1, 2, 3):
                dispatch_copy(s, r).wait_recv()
        far = x_buf[SEG:, :].astype(f32)
        if s < N_SEG:
            far = far + recv[s, :3 * SEG, :].astype(f32) * (hot_slot > s).astype(f32)
        if s > 0:
            far = far + recv[s - 1, :3 * SEG, :].astype(f32) * (hot_slot < s).astype(f32)
        x_buf[SEG:, :] = far.astype(bf16)
        for copy in weight_copies(s):
            copy.wait()
        b = s % N_WBUF
        acc[...] = jnp.zeros_like(acc)

        def ff_step(i, carry):
            cols = pl.ds(pl.multiple_of(i * FF_TILE, FF_TILE), FF_TILE)
            pre = jnp.dot(x_buf[...], up_buf[b, :, cols], preferred_element_type=f32)
            hidden = jax.nn.gelu(pre, approximate=True).astype(bf16)
            acc[...] += jnp.dot(hidden, down_buf[b, cols, :], preferred_element_type=f32)
            return carry

        lax.fori_loop(0, d_ff // FF_TILE, ff_step, 0)
        if s + N_WBUF < n_slot:
            for copy in weight_copies(s + N_WBUF):
                copy.start()
        result[s * SLOT_ROWS:(s + 1) * SLOT_ROWS, :] = acc[...].astype(bf16)
        if s > 0:
            k = s - 1
            prev = result[k * SLOT_ROWS + SEG:(k + 1) * SLOT_ROWS, :].astype(f32)
            back = prev * (hot_slot > k).astype(f32) + acc[SEG:, :].astype(bf16).astype(f32) * (hot_slot <= k).astype(f32)
            back_send[k, :3 * SEG, :] = back.astype(bf16)
            for r in (2, 3, 1):
                back_copy(k, r).start()

    tile = 256

    def combine(first, rows, source, add):
        def body(i, carry):
            at = pl.ds(pl.multiple_of(i * tile, tile), tile)
            mine = code_col[at, :]
            ids = lax.broadcasted_iota(jnp.int32, (tile, 128), 1) + first
            mask = jnp.concatenate([(mine == ids + 128 * j).astype(f32).astype(bf16) for j in range(rows // 128)], axis=1)
            part = jnp.dot(mask, source(), preferred_element_type=f32)
            if add:
                part = part + out[at, :].astype(f32)
            out[at, :] = part.astype(bf16)
            return carry
        lax.fori_loop(0, n_tok // tile, body, 0)

    combine(LOCAL_BASE, LOCAL_ROWS, lambda: result[...], False)
    for k in range(N_SEG):
        for r in (1, 2, 3):
            back_copy(k, r).wait_recv()
        combine(k * SEG_ROWS, SEG_ROWS, lambda: back_recv[k], True)
    for k in range(N_SEG):
        for r in (1, 2, 3):
            dispatch_copy(k, r).wait_send()
            back_copy(k, r).wait_send()


def fast_layer(tokens, topk_idx, w_up, w_down, slot_expert):
    n_tok, d_model = tokens.shape
    n_slot, d_ff = w_up.shape[1], w_up.shape[3]
    vmem = pl.BlockSpec(memory_space=pltpu.VMEM)
    anym = pl.BlockSpec(memory_space=pl.ANY)
    bf16 = jnp.bfloat16
    return pl.pallas_call(
        layer_kernel,
        out_shape=jax.ShapeDtypeStruct((n_tok, d_model), bf16),
        in_specs=[pl.BlockSpec(memory_space=pltpu.SMEM), vmem, vmem, anym, anym],
        out_specs=vmem,
        scratch_shapes=[
            pltpu.VMEM((N_WBUF, d_model, d_ff), bf16),
            pltpu.VMEM((N_WBUF, d_ff, d_model), bf16),
            pltpu.VMEM((N_SEG, SEG_ROWS, d_model), bf16),
            pltpu.VMEM((N_SEG, SEG_ROWS, d_model), bf16),
            pltpu.VMEM((SLOT_ROWS, d_model), bf16),
            pltpu.VMEM((SLOT_ROWS, d_model), jnp.float32),
            pltpu.VMEM((LOCAL_ROWS, d_model), bf16),
            pltpu.VMEM((N_SEG, SEG_ROWS, d_model), bf16),
            pltpu.VMEM((N_SEG, SEG_ROWS, d_model), bf16),
            pltpu.VMEM((8, n_tok), jnp.int32),
            pltpu.VMEM((n_tok, 128), jnp.int32),
            pltpu.SemaphoreType.DMA((n_slot, 2)),
            pltpu.SemaphoreType.DMA((N_SEG, 3)),
            pltpu.SemaphoreType.DMA((N_SEG, 3)),
            pltpu.SemaphoreType.DMA((N_SEG, 3)),
            pltpu.SemaphoreType.DMA((N_SEG, 3)),
        ],
        compiler_params=pltpu.CompilerParams(collective_id=0, has_side_effects=True, vmem_limit_bytes=60 * 1024 * 1024),
    )(slot_expert, tokens, topk_idx.reshape(1, n_tok), w_up[0], w_down[0])


def solution(mesh):
    def group_layer(tokens, topk_idx, topk_w, w_up, w_down, slot_expert):
        flat = slot_expert.reshape(-1)
        copies = jnp.sum(flat[:, None] == flat[None, :], axis=1)
        pair_out = lax.cond(jnp.any(copies == 4), fast_layer, general_layer, tokens, topk_idx, w_up, w_down, slot_expert)
        return (pair_out.astype(jnp.float32) * topk_w).astype(jnp.bfloat16)

    row_spec = P(('dp', 'ep'), None)
    weight_spec = P('ep', None, None, None)
    return jax.shard_map(group_layer, mesh=mesh, in_specs=(row_spec, row_spec, row_spec, weight_spec, weight_spec, P(None, None)), out_specs=row_spec, check_vma=False)
```

```python
import functools

import jax
import jax.numpy as jnp
from jax import lax
from jax.experimental import pallas as pl
from jax.experimental.pallas import tpu as pltpu
from jax.sharding import PartitionSpec as P

MAX_COPIES = 4
SEG = 80
N_SEG = 4
SEG_ROWS = 256
SLOT_ROWS = 4 * SEG
LOCAL_BASE = N_SEG * SEG_ROWS
LOCAL_ROWS = 1664
FF_TILE = 512
N_WBUF = 4
MESH = pl.DeviceIdType.MESH


def slot_bound(n_tok, n_top, n_dev, n_slot):
    base_load = (n_tok * n_top) // (n_dev * n_slot)
    return base_load + base_load // 2 + 1


def route_pairs(topk_idx, slot_expert, capacity):
    n_dev, n_slot = slot_expert.shape
    n_exp = n_dev * (n_slot - 1)
    n_top = topk_idx.shape[1]
    table_flat = slot_expert.reshape(-1)
    slot_ids = jnp.arange(n_dev * n_slot, dtype=jnp.int32)
    same_exp = table_flat[:, None] == table_flat[None, :]
    earlier = slot_ids[None, :] < slot_ids[:, None]
    copy_rank = jnp.sum(same_exp & earlier, axis=1, dtype=jnp.int32)
    exp_copies = jax.ops.segment_sum(jnp.ones_like(table_flat), table_flat, num_segments=n_exp)
    slot_of = jnp.zeros((n_exp, MAX_COPIES), jnp.int32).at[table_flat, copy_rank].set(slot_ids)
    flat_exp = topk_idx.reshape(-1)
    onehot = (flat_exp[:, None] == jnp.arange(n_exp, dtype=jnp.int32)[None, :]).astype(jnp.int32)
    pair_rank = jnp.sum((jnp.cumsum(onehot, axis=0) - onehot) * onehot, axis=1)
    pair_copies = exp_copies[flat_exp]
    slot_flat = slot_of[flat_exp, pair_rank % pair_copies]
    buf_row = pair_rank // pair_copies
    pair_pos = ((slot_flat % n_slot) * n_dev + slot_flat // n_slot) * capacity + buf_row
    pair_tok = jnp.arange(flat_exp.shape[0], dtype=jnp.int32) // n_top
    buf_tok = jnp.zeros((n_slot * n_dev * capacity,), jnp.int32).at[pair_pos].set(pair_tok)
    return pair_pos, buf_tok


def expert_ffn(recv_buf, up_local, down_local):
    pre_act = jnp.einsum('spcm,smf->spcf', recv_buf, up_local, preferred_element_type=jnp.float32)
    hidden = jax.nn.gelu(pre_act, approximate=True).astype(jnp.bfloat16)
    return jnp.einsum('spcf,sfm->spcm', hidden, down_local, preferred_element_type=jnp.float32).astype(jnp.bfloat16)


def general_layer(tokens, topk_idx, topk_w, w_up, w_down, slot_expert):
    n_tok, d_model = tokens.shape
    n_top = topk_idx.shape[1]
    n_dev, n_slot = slot_expert.shape
    capacity = slot_bound(n_tok, n_top, n_dev, n_slot)
    pair_pos, buf_tok = route_pairs(topk_idx, slot_expert, capacity)
    send_buf = tokens[buf_tok].reshape(n_slot, n_dev, capacity, d_model)
    recv_buf = lax.all_to_all(send_buf, 'ep', 1, 1, tiled=True)
    expert_out = expert_ffn(recv_buf, w_up[0], w_down[0])
    back_buf = lax.all_to_all(expert_out, 'ep', 1, 1, tiled=True)
    pair_out = back_buf.reshape(-1, d_model)[pair_pos]
    return (pair_out.astype(jnp.float32) * topk_w).astype(jnp.bfloat16)


def route(idx_row, table, peers, n_exp, n_slot):
    f32 = jnp.float32
    n_tok = idx_row.shape[1]
    lanes = 128
    exp_id = lax.broadcasted_iota(jnp.int32, (n_exp, lanes), 0)
    match = [[(exp_id == table[d, s]).astype(f32) for s in range(n_slot)] for d in peers]
    copies = sum(sum(row) for row in match)
    hot = (copies == 4.0).astype(f32)
    own = sum(match[0])
    own_slot = sum(s * match[0][s] for s in range(n_slot))
    seen = jnp.zeros((n_exp, lanes), f32)
    base = [jnp.zeros((n_exp, lanes), f32) for _ in range(MAX_COPIES)]
    for r in range(len(peers)):
        passed = jnp.zeros((1, lanes), f32)
        for s in range(n_slot):
            here = match[r][s]
            local = LOCAL_BASE + SLOT_ROWS * own_slot + SEG * r
            if r == 0:
                code = local
            else:
                seg = s - passed
                code = jnp.where(own > 0, local, SEG_ROWS * seg + SEG * (r - 1))
                passed = passed + jnp.sum(here * hot, axis=0, keepdims=True)
            for c in range(MAX_COPIES):
                base[c] = jnp.where((here > 0) & (seen == c), code, base[c])
            seen = seen + here
    hot_slot = sum(s * jnp.sum(match[0][s] * hot, axis=0, keepdims=True) for s in range(n_slot))

    wide = lambda a: jnp.concatenate([a] * (n_tok // lanes), axis=1)
    onehot = (lax.broadcasted_iota(jnp.int32, (n_exp, n_tok), 0) == idx_row).astype(f32)
    step = 256
    blocks = [onehot[:, b * step:(b + 1) * step] for b in range(n_tok // step)]
    before = lax.broadcasted_iota(jnp.int32, (step, step), 0) < lax.broadcasted_iota(jnp.int32, (step, step), 1)
    local_rank = jnp.dot(jnp.concatenate(blocks, axis=0).astype(jnp.bfloat16), before.astype(f32).astype(jnp.bfloat16), preferred_element_type=f32)
    carry = jnp.zeros((n_exp, 1), f32)
    ranks = []
    for b, block in enumerate(blocks):
        ranks.append(local_rank[b * n_exp:(b + 1) * n_exp] + carry)
        carry = carry + jnp.sum(block, axis=1, keepdims=True)
    rank = jnp.concatenate(ranks, axis=1)
    n_copy = wide(copies)
    row = jnp.floor((rank + 0.5) * wide(1.0 / copies))
    which = rank - row * n_copy
    start = wide(base[3])
    for c in range(MAX_COPIES - 1):
        start = jnp.where(which == c, wide(base[c]), start)
    code = jnp.sum(onehot * (start + row), axis=0, keepdims=True)
    return code.astype(jnp.int32), hot_slot


def layer_kernel(table, idx_row, gate_row, tokens, w_up, w_down, out, found, tok_buf, up_buf, down_buf, send, recv, acc, rows_buf, back_send, back_recv, mixed, code_row, code_col, gate_col, t_sem, w_sem, ds_sem, dr_sem, bs_sem, br_sem, o_sem):
    f32, bf16 = jnp.float32, jnp.bfloat16
    n_tok, d_model = tok_buf.shape
    n_slot = w_up.shape[0]
    d_ff = w_up.shape[2]
    me = lax.axis_index('ep')
    chip, core = me // 2, me % 2
    peers = [me, 2 * chip + (1 - core), 2 * (1 - chip) + core, 2 * (1 - chip) + (1 - core)]

    barrier = pltpu.get_barrier_semaphore()
    for r in (1, 2, 3):
        pl.semaphore_signal(barrier, inc=1, device_id={'ep': peers[r]}, device_id_type=MESH)

    def weight_copies(s):
        b = s % N_WBUF
        return (pltpu.make_async_copy(w_up.at[s], up_buf.at[b], w_sem.at[s, 0]),
                pltpu.make_async_copy(w_down.at[s], down_buf.at[b], w_sem.at[s, 1]))

    token_copy = pltpu.make_async_copy(tokens, tok_buf, t_sem)
    token_copy.start()
    for s in range(N_WBUF):
        for copy in weight_copies(s):
            copy.start()

    code, hot_slot = route(idx_row[...], table, peers, 16, n_slot)
    code_row[...] = jnp.broadcast_to(code, code_row.shape)
    hot_slot = hot_slot[:, :1]

    def pick(first, rows):
        ids = lax.broadcasted_iota(jnp.int32, (rows, n_tok), 0) + first
        mask = (ids == code_row[0:1, :]).astype(f32).astype(bf16)
        return jnp.dot(mask, tok_buf[...], preferred_element_type=f32).astype(bf16)

    def dispatch_copy(k, r):
        rows = pl.ds((r - 1) * SEG, SEG)
        return pltpu.make_async_remote_copy(
            src_ref=send.at[k, rows], dst_ref=recv.at[k, rows],
            send_sem=ds_sem.at[k, r - 1], recv_sem=dr_sem.at[k, r - 1],
            device_id={'ep': peers[r]}, device_id_type=MESH)

    def back_copy(k, r):
        rows = pl.ds((r - 1) * SEG, SEG)
        return pltpu.make_async_remote_copy(
            src_ref=back_send.at[k, rows], dst_ref=back_recv.at[k, rows],
            send_sem=bs_sem.at[k, r - 1], recv_sem=br_sem.at[k, r - 1],
            device_id={'ep': peers[r]}, device_id_type=MESH)

    token_copy.wait()
    for k in range(N_SEG):
        send[k] = pick(k * SEG_ROWS, SEG_ROWS)
        if k == 0:
            pl.semaphore_wait(barrier, 3)
        for r in (2, 3, 1):
            dispatch_copy(k, r).start()

    for s in range(n_slot):
        rows_buf[s * SLOT_ROWS:(s + 1) * SLOT_ROWS, :] = pick(LOCAL_BASE + s * SLOT_ROWS, SLOT_ROWS)
    code_col[...] = jnp.transpose(jnp.broadcast_to(code, (128, n_tok)))
    gate_col[...] = jnp.transpose(jnp.broadcast_to(gate_row[...], (128, n_tok)))
    back_recv[:, 3 * SEG:, :] = jnp.zeros((N_SEG, SEG_ROWS - 3 * SEG, d_model), bf16)
    rows_buf[n_slot * SLOT_ROWS:, :] = jnp.zeros((LOCAL_ROWS - n_slot * SLOT_ROWS, d_model), bf16)
    hot = jnp.int32(0)
    for s in range(n_slot):
        here = sum((table[d, q] == table[me, s]).astype(jnp.int32) for d in range(4) for q in range(n_slot))
        hot = hot | (here == 4).astype(jnp.int32)
    found[0, 0] = hot

    for s in range(n_slot):
        lo, hi = s * SLOT_ROWS, (s + 1) * SLOT_ROWS
        if s < N_SEG:
            for r in (1, 2, 3):
                dispatch_copy(s, r).wait_recv()
        far = rows_buf[lo + SEG:hi, :].astype(f32)
        if s < N_SEG:
            far = far + recv[s, :3 * SEG, :].astype(f32) * (hot_slot > s).astype(f32)
        if s > 0:
            far = far + recv[s - 1, :3 * SEG, :].astype(f32) * (hot_slot < s).astype(f32)
        rows_buf[lo + SEG:hi, :] = far.astype(bf16)
        for copy in weight_copies(s):
            copy.wait()
        b = s % N_WBUF
        acc[...] = jnp.zeros_like(acc)

        def ff_step(i, carry):
            cols = pl.ds(pl.multiple_of(i * FF_TILE, FF_TILE), FF_TILE)
            pre = jnp.dot(rows_buf[lo:hi, :], up_buf[b, :, cols], preferred_element_type=f32)
            hidden = jax.nn.gelu(pre, approximate=True).astype(bf16)
            acc[...] += jnp.dot(hidden, down_buf[b, cols, :], preferred_element_type=f32)
            return carry

        lax.fori_loop(0, d_ff // FF_TILE, ff_step, 0)
        if s + N_WBUF < n_slot:
            for copy in weight_copies(s + N_WBUF):
                copy.start()
        rows_buf[lo:hi, :] = acc[...].astype(bf16)
        if s > 0:
            k = s - 1
            prev = rows_buf[lo - SLOT_ROWS + SEG:lo, :].astype(f32)
            last = rows_buf[lo + SEG:hi, :].astype(f32)
            back = prev * (hot_slot > k).astype(f32) + last * (hot_slot <= k).astype(f32)
            back_send[k, :3 * SEG, :] = back.astype(bf16)
            for r in (2, 3, 1):
                back_copy(k, r).start()

    tile = 256
    n_tile = n_tok // tile

    def out_copy(i):
        at = pl.ds(pl.multiple_of(i * tile, tile), tile)
        return pltpu.make_async_copy(mixed.at[at], out.at[at], o_sem.at[i])

    def combine(first, rows, source, add, final):
        def body(i, carry):
            at = pl.ds(pl.multiple_of(i * tile, tile), tile)
            mine = code_col[at, :]
            ids = lax.broadcasted_iota(jnp.int32, (tile, 128), 1) + first
            mask = jnp.concatenate([(mine == ids + 128 * j).astype(f32).astype(bf16) for j in range(rows // 128)], axis=1)
            part = jnp.dot(mask, source(), preferred_element_type=f32)
            if add:
                part = part + mixed[at, :].astype(f32)
            if final:
                part = part * jnp.concatenate([gate_col[at, :]] * (d_model // 128), axis=1)
            mixed[at, :] = part.astype(bf16)
            if final:
                out_copy(i).start()
            return carry
        lax.fori_loop(0, n_tile, body, 0)

    combine(LOCAL_BASE, LOCAL_ROWS, lambda: rows_buf[...], False, False)
    for k in range(N_SEG):
        for r in (1, 2, 3):
            back_copy(k, r).wait_recv()
        combine(k * SEG_ROWS, SEG_ROWS, lambda: back_recv[k], True, k == N_SEG - 1)
    for k in range(N_SEG):
        for r in (1, 2, 3):
            dispatch_copy(k, r).wait_send()
            back_copy(k, r).wait_send()
    for i in range(n_tile):
        out_copy(i).wait()


def fast_layer(tokens, topk_idx, topk_w, w_up, w_down, slot_expert):
    n_tok, d_model = tokens.shape
    n_slot, d_ff = w_up.shape[1], w_up.shape[3]
    vmem = pl.BlockSpec(memory_space=pltpu.VMEM)
    smem = pl.BlockSpec(memory_space=pltpu.SMEM)
    anym = pl.BlockSpec(memory_space=pl.ANY)
    bf16 = jnp.bfloat16
    return pl.pallas_call(
        layer_kernel,
        out_shape=(jax.ShapeDtypeStruct((n_tok, d_model), bf16), jax.ShapeDtypeStruct((1, 1), jnp.int32)),
        in_specs=[smem, vmem, vmem, anym, anym, anym],
        out_specs=(anym, smem),
        scratch_shapes=[
            pltpu.VMEM((n_tok, d_model), bf16),
            pltpu.VMEM((N_WBUF, d_model, d_ff), bf16),
            pltpu.VMEM((N_WBUF, d_ff, d_model), bf16),
            pltpu.VMEM((N_SEG, SEG_ROWS, d_model), bf16),
            pltpu.VMEM((N_SEG, SEG_ROWS, d_model), bf16),
            pltpu.VMEM((SLOT_ROWS, d_model), jnp.float32),
            pltpu.VMEM((LOCAL_ROWS, d_model), bf16),
            pltpu.VMEM((N_SEG, SEG_ROWS, d_model), bf16),
            pltpu.VMEM((N_SEG, SEG_ROWS, d_model), bf16),
            pltpu.VMEM((n_tok, d_model), bf16),
            pltpu.VMEM((8, n_tok), jnp.int32),
            pltpu.VMEM((n_tok, 128), jnp.int32),
            pltpu.VMEM((n_tok, 128), jnp.float32),
            pltpu.SemaphoreType.DMA,
            pltpu.SemaphoreType.DMA((n_slot, 2)),
            pltpu.SemaphoreType.DMA((N_SEG, 3)),
            pltpu.SemaphoreType.DMA((N_SEG, 3)),
            pltpu.SemaphoreType.DMA((N_SEG, 3)),
            pltpu.SemaphoreType.DMA((N_SEG, 3)),
            pltpu.SemaphoreType.DMA((n_tok // 256,)),
        ],
        compiler_params=pltpu.CompilerParams(collective_id=0, has_side_effects=True, vmem_limit_bytes=60 * 1024 * 1024),
    )(slot_expert, topk_idx.reshape(1, n_tok), topk_w.reshape(1, n_tok), tokens, w_up[0], w_down[0])


def solution(mesh):
    def group_layer(tokens, topk_idx, topk_w, w_up, w_down, slot_expert):
        fast_out, found = fast_layer(tokens, topk_idx, topk_w, w_up, w_down, slot_expert)
        args = (fast_out, tokens, topk_idx, topk_w, w_up, w_down, slot_expert)
        return lax.cond(found[0, 0] == 1, lambda *a: a[0], lambda *a: general_layer(*a[1:]), *args)

    row_spec = P(('dp', 'ep'), None)
    weight_spec = P('ep', None, None, None)
    return jax.shard_map(group_layer, mesh=mesh, in_specs=(row_spec, row_spec, row_spec, weight_spec, weight_spec, P(None, None)), out_specs=row_spec, check_vma=False)
```

```python
import functools

import jax
import jax.numpy as jnp
from jax import lax
from jax.experimental import pallas as pl
from jax.experimental.pallas import tpu as pltpu
from jax.sharding import PartitionSpec as P

MAX_COPIES = 4
SEG = 80
N_SEG = 4
SEG_ROWS = 256
SLOT_ROWS = 4 * SEG
LOCAL_BASE = N_SEG * SEG_ROWS
LOCAL_ROWS = 1664
FF_TILE = 512
N_WBUF = 4
MESH = pl.DeviceIdType.MESH


def slot_bound(n_tok, n_top, n_dev, n_slot):
    base_load = (n_tok * n_top) // (n_dev * n_slot)
    return base_load + base_load // 2 + 1


def route_pairs(topk_idx, slot_expert, capacity):
    n_dev, n_slot = slot_expert.shape
    n_exp = n_dev * (n_slot - 1)
    n_top = topk_idx.shape[1]
    table_flat = slot_expert.reshape(-1)
    slot_ids = jnp.arange(n_dev * n_slot, dtype=jnp.int32)
    same_exp = table_flat[:, None] == table_flat[None, :]
    earlier = slot_ids[None, :] < slot_ids[:, None]
    copy_rank = jnp.sum(same_exp & earlier, axis=1, dtype=jnp.int32)
    exp_copies = jax.ops.segment_sum(jnp.ones_like(table_flat), table_flat, num_segments=n_exp)
    slot_of = jnp.zeros((n_exp, MAX_COPIES), jnp.int32).at[table_flat, copy_rank].set(slot_ids)
    flat_exp = topk_idx.reshape(-1)
    onehot = (flat_exp[:, None] == jnp.arange(n_exp, dtype=jnp.int32)[None, :]).astype(jnp.int32)
    pair_rank = jnp.sum((jnp.cumsum(onehot, axis=0) - onehot) * onehot, axis=1)
    pair_copies = exp_copies[flat_exp]
    slot_flat = slot_of[flat_exp, pair_rank % pair_copies]
    buf_row = pair_rank // pair_copies
    pair_pos = ((slot_flat % n_slot) * n_dev + slot_flat // n_slot) * capacity + buf_row
    pair_tok = jnp.arange(flat_exp.shape[0], dtype=jnp.int32) // n_top
    buf_tok = jnp.zeros((n_slot * n_dev * capacity,), jnp.int32).at[pair_pos].set(pair_tok)
    return pair_pos, buf_tok


def expert_ffn(recv_buf, up_local, down_local):
    pre_act = jnp.einsum('spcm,smf->spcf', recv_buf, up_local, preferred_element_type=jnp.float32)
    hidden = jax.nn.gelu(pre_act, approximate=True).astype(jnp.bfloat16)
    return jnp.einsum('spcf,sfm->spcm', hidden, down_local, preferred_element_type=jnp.float32).astype(jnp.bfloat16)


def general_layer(tokens, topk_idx, topk_w, w_up, w_down, slot_expert):
    n_tok, d_model = tokens.shape
    n_top = topk_idx.shape[1]
    n_dev, n_slot = slot_expert.shape
    capacity = slot_bound(n_tok, n_top, n_dev, n_slot)
    pair_pos, buf_tok = route_pairs(topk_idx, slot_expert, capacity)
    send_buf = tokens[buf_tok].reshape(n_slot, n_dev, capacity, d_model)
    recv_buf = lax.all_to_all(send_buf, 'ep', 1, 1, tiled=True)
    expert_out = expert_ffn(recv_buf, w_up[0], w_down[0])
    back_buf = lax.all_to_all(expert_out, 'ep', 1, 1, tiled=True)
    pair_out = back_buf.reshape(-1, d_model)[pair_pos]
    return (pair_out.astype(jnp.float32) * topk_w).astype(jnp.bfloat16)


def route(idx_row, table, peers, n_exp, n_slot):
    f32 = jnp.float32
    n_tok = idx_row.shape[1]
    lanes = 128
    exp_id = lax.broadcasted_iota(jnp.int32, (n_exp, lanes), 0)
    match = [[(exp_id == table[d, s]).astype(f32) for s in range(n_slot)] for d in peers]
    copies = sum(sum(row) for row in match)
    hot = (copies == 4.0).astype(f32)
    own = sum(match[0])
    own_slot = sum(s * match[0][s] for s in range(n_slot))
    seen = jnp.zeros((n_exp, lanes), f32)
    base = [jnp.zeros((n_exp, lanes), f32) for _ in range(MAX_COPIES)]
    for r in range(len(peers)):
        passed = jnp.zeros((1, lanes), f32)
        for s in range(n_slot):
            here = match[r][s]
            local = LOCAL_BASE + SLOT_ROWS * own_slot + SEG * r
            if r == 0:
                code = local
            else:
                seg = s - passed
                code = jnp.where(own > 0, local, SEG_ROWS * seg + SEG * (r - 1))
                passed = passed + jnp.sum(here * hot, axis=0, keepdims=True)
            for c in range(MAX_COPIES):
                base[c] = jnp.where((here > 0) & (seen == c), code, base[c])
            seen = seen + here
    hot_slot = sum(s * jnp.sum(match[0][s] * hot, axis=0, keepdims=True) for s in range(n_slot))

    wide = lambda a: jnp.concatenate([a] * (n_tok // lanes), axis=1)
    onehot = (lax.broadcasted_iota(jnp.int32, (n_exp, n_tok), 0) == idx_row).astype(f32)
    step = 256
    blocks = [onehot[:, b * step:(b + 1) * step] for b in range(n_tok // step)]
    before = lax.broadcasted_iota(jnp.int32, (step, step), 0) < lax.broadcasted_iota(jnp.int32, (step, step), 1)
    local_rank = jnp.dot(jnp.concatenate(blocks, axis=0).astype(jnp.bfloat16), before.astype(f32).astype(jnp.bfloat16), preferred_element_type=f32)
    carry = jnp.zeros((n_exp, 1), f32)
    ranks = []
    for b, block in enumerate(blocks):
        ranks.append(local_rank[b * n_exp:(b + 1) * n_exp] + carry)
        carry = carry + jnp.sum(block, axis=1, keepdims=True)
    rank = jnp.concatenate(ranks, axis=1)
    n_copy = wide(copies)
    row = jnp.floor((rank + 0.5) * wide(1.0 / copies))
    which = rank - row * n_copy
    start = wide(base[3])
    for c in range(MAX_COPIES - 1):
        start = jnp.where(which == c, wide(base[c]), start)
    code = jnp.sum(onehot * (start + row), axis=0, keepdims=True)
    return code.astype(jnp.int32), hot_slot, jnp.max(own * hot, axis=0, keepdims=True)


def layer_kernel(slot_expert, topk_idx, topk_w, tokens, w_up, w_down, out, last_rows, last_mask, last_gate, found, table, idx_row, gate_row, tok_buf, up_buf, down_buf, send, recv, acc, rows_buf, back_send, back_recv, mixed, mask_buf, gate_buf, code_row, code_col, gate_col, t_sem, w_sem, ds_sem, dr_sem, bs_sem, br_sem, o_sem):
    f32, bf16 = jnp.float32, jnp.bfloat16
    n_tok, d_model = tok_buf.shape
    n_slot = w_up.shape[0]
    d_ff = w_up.shape[2]
    me = lax.axis_index('ep')
    chip, core = me // 2, me % 2
    peers = [me, 2 * chip + (1 - core), 2 * (1 - chip) + core, 2 * (1 - chip) + (1 - core)]

    barrier = pltpu.get_barrier_semaphore()
    for r in (1, 2, 3):
        pl.semaphore_signal(barrier, inc=1, device_id={'ep': peers[r]}, device_id_type=MESH)

    def weight_copies(s):
        b = s % N_WBUF
        return (pltpu.make_async_copy(w_up.at[s], up_buf.at[b], w_sem.at[s, 0]),
                pltpu.make_async_copy(w_down.at[s], down_buf.at[b], w_sem.at[s, 1]))

    small_copies = [pltpu.make_async_copy(slot_expert, table, t_sem.at[0]),
                    pltpu.make_async_copy(topk_idx, idx_row, t_sem.at[1]),
                    pltpu.make_async_copy(topk_w, gate_row, t_sem.at[2])]
    token_copy = pltpu.make_async_copy(tokens, tok_buf, t_sem.at[3])
    for copy in small_copies:
        copy.start()
    token_copy.start()
    for copy in small_copies:
        copy.wait()
    code, hot_slot, hot_here = route(idx_row[...], table, peers, 16, n_slot)
    code_row[...] = jnp.broadcast_to(code, code_row.shape)
    hot_slot = hot_slot[:, :1]

    def pick(first, rows):
        ids = lax.broadcasted_iota(jnp.int32, (rows, n_tok), 0) + first
        mask = (ids == code_row[0:1, :]).astype(f32).astype(bf16)
        return jnp.dot(mask, tok_buf[...], preferred_element_type=f32).astype(bf16)

    def dispatch_copy(k, r):
        rows = pl.ds((r - 1) * SEG, SEG)
        return pltpu.make_async_remote_copy(
            src_ref=send.at[k, rows], dst_ref=recv.at[k, rows],
            send_sem=ds_sem.at[k, r - 1], recv_sem=dr_sem.at[k, r - 1],
            device_id={'ep': peers[r]}, device_id_type=MESH)

    def back_copy(k, r):
        rows = pl.ds((r - 1) * SEG, SEG)
        return pltpu.make_async_remote_copy(
            src_ref=back_send.at[k, rows], dst_ref=back_recv.at[k, rows] if k < N_SEG - 1 else last_rows.at[rows],
            send_sem=bs_sem.at[k, r - 1], recv_sem=br_sem.at[k, r - 1],
            device_id={'ep': peers[r]}, device_id_type=MESH)

    token_copy.wait()
    for s in range(N_WBUF):
        for copy in weight_copies(s):
            copy.start()
    for k in range(N_SEG):
        send[k] = pick(k * SEG_ROWS, SEG_ROWS)
        if k == 0:
            pl.semaphore_wait(barrier, 3)
        for r in (2, 3, 1):
            dispatch_copy(k, r).start()

    for s in range(n_slot):
        rows_buf[s * SLOT_ROWS:(s + 1) * SLOT_ROWS, :] = pick(LOCAL_BASE + s * SLOT_ROWS, SLOT_ROWS)
    code_col[...] = jnp.transpose(jnp.broadcast_to(code, (128, n_tok)))
    gate_col[...] = jnp.transpose(jnp.broadcast_to(gate_row[...], (128, n_tok)))
    back_recv[:, 3 * SEG:, :] = jnp.zeros((N_SEG - 1, SEG_ROWS - 3 * SEG, d_model), bf16)
    rows_buf[n_slot * SLOT_ROWS:, :] = jnp.zeros((LOCAL_ROWS - n_slot * SLOT_ROWS, d_model), bf16)
    found[...] = jnp.broadcast_to(hot_here.astype(jnp.int32), found.shape)
    last = (N_SEG - 1) * SEG_ROWS
    ids = lax.broadcasted_iota(jnp.int32, (3 * SEG, n_tok), 0) + last
    gates = jnp.sum(jnp.where(ids == code_row[0:1, :], gate_row[...], 0.0), axis=1, keepdims=True)
    gate_buf[...] = jnp.broadcast_to(gates, gate_buf.shape)
    ids = lax.broadcasted_iota(jnp.int32, (n_tok, 128), 1) + last
    for j in range(SEG_ROWS // 128):
        mask_buf[:, j * 128:(j + 1) * 128] = (code_col[...] == ids + 128 * j).astype(f32).astype(bf16)
    side_copies = [pltpu.make_async_copy(mask_buf, last_mask, t_sem.at[4]),
                   pltpu.make_async_copy(gate_buf, last_gate, t_sem.at[5])]
    for copy in side_copies:
        copy.start()

    for s in range(n_slot):
        lo, hi = s * SLOT_ROWS, (s + 1) * SLOT_ROWS
        if s < N_SEG:
            for r in (1, 2, 3):
                dispatch_copy(s, r).wait_recv()
        far = rows_buf[lo + SEG:hi, :].astype(f32)
        if s < N_SEG:
            far = far + recv[s, :3 * SEG, :].astype(f32) * (hot_slot > s).astype(f32)
        if s > 0:
            far = far + recv[s - 1, :3 * SEG, :].astype(f32) * (hot_slot < s).astype(f32)
        rows_buf[lo + SEG:hi, :] = far.astype(bf16)
        for copy in weight_copies(s):
            copy.wait()
        b = s % N_WBUF
        acc[...] = jnp.zeros_like(acc)

        def ff_step(i, carry):
            cols = pl.ds(pl.multiple_of(i * FF_TILE, FF_TILE), FF_TILE)
            pre = jnp.dot(rows_buf[lo:hi, :], up_buf[b, :, cols], preferred_element_type=f32)
            hidden = jax.nn.gelu(pre, approximate=True).astype(bf16)
            acc[...] += jnp.dot(hidden, down_buf[b, cols, :], preferred_element_type=f32)
            return carry

        lax.fori_loop(0, d_ff // FF_TILE, ff_step, 0)
        if s + N_WBUF < n_slot:
            for copy in weight_copies(s + N_WBUF):
                copy.start()
        rows_buf[lo:hi, :] = acc[...].astype(bf16)
        if s > 0:
            k = s - 1
            prev = rows_buf[lo - SLOT_ROWS + SEG:lo, :].astype(f32)
            last = rows_buf[lo + SEG:hi, :].astype(f32)
            back = prev * (hot_slot > k).astype(f32) + last * (hot_slot <= k).astype(f32)
            back_send[k, :3 * SEG, :] = back.astype(bf16)
            for r in (2, 3, 1):
                back_copy(k, r).start()

    tile = 256
    n_tile = n_tok // tile

    def out_copy(i):
        at = pl.ds(pl.multiple_of(i * tile, tile), tile)
        return pltpu.make_async_copy(mixed.at[at], out.at[at], o_sem.at[i])

    def combine(first, rows, source, add, final):
        def body(i, carry):
            at = pl.ds(pl.multiple_of(i * tile, tile), tile)
            mine = code_col[at, :]
            ids = lax.broadcasted_iota(jnp.int32, (tile, 128), 1) + first
            mask = jnp.concatenate([(mine == ids + 128 * j).astype(f32).astype(bf16) for j in range(rows // 128)], axis=1)
            part = jnp.dot(mask, source(), preferred_element_type=f32)
            if add:
                part = part + mixed[at, :].astype(f32)
            if final:
                part = part * jnp.concatenate([gate_col[at, :]] * (d_model // 128), axis=1)
            mixed[at, :] = part.astype(bf16)
            if final:
                out_copy(i).start()
            return carry
        lax.fori_loop(0, n_tile, body, 0)

    combine(LOCAL_BASE, LOCAL_ROWS, lambda: rows_buf[...], False, False)
    for k in range(N_SEG):
        for r in (1, 2, 3):
            back_copy(k, r).wait_recv()
        if k < N_SEG - 1:
            combine(k * SEG_ROWS, SEG_ROWS, lambda: back_recv[k], True, k == N_SEG - 2)
        if k == N_SEG - 2:
            for i in range(n_tile):
                out_copy(i).wait()
            for copy in side_copies:
                copy.wait()
    for k in range(N_SEG):
        for r in (1, 2, 3):
            dispatch_copy(k, r).wait_send()
            back_copy(k, r).wait_send()


def last_kernel(part, rows, mask, gate, out):
    f32, bf16 = jnp.float32, jnp.bfloat16
    d_model = part.shape[1]
    gates = jnp.concatenate([gate[...]] * (d_model // 128), axis=1)
    scaled = (rows[...].astype(f32) * gates).astype(bf16)
    scaled = jnp.concatenate([scaled, jnp.zeros((SEG_ROWS - scaled.shape[0], d_model), bf16)], axis=0)
    late = jnp.dot(mask[...], scaled, preferred_element_type=f32)
    out[...] = (late + part[...].astype(f32)).astype(bf16)


def add_last(part, rows, mask, gate):
    n_tok, d_model = part.shape
    tile = 256
    by_tile = lambda cols: pl.BlockSpec((tile, cols), lambda i: (i, 0))
    whole = lambda a: pl.BlockSpec(a.shape, lambda i: (0, 0))
    return pl.pallas_call(
        last_kernel,
        grid=(n_tok // tile,),
        out_shape=jax.ShapeDtypeStruct(part.shape, part.dtype),
        in_specs=[by_tile(d_model), whole(rows), by_tile(mask.shape[1]), whole(gate)],
        out_specs=by_tile(d_model),
    )(part, rows, mask, gate)


def fast_layer(tokens, topk_idx, topk_w, w_up, w_down, slot_expert):
    n_tok, d_model = tokens.shape
    n_slot, d_ff = w_up.shape[1], w_up.shape[3]
    vmem = pl.BlockSpec(memory_space=pltpu.VMEM)
    anym = pl.BlockSpec(memory_space=pl.ANY)
    bf16 = jnp.bfloat16
    return pl.pallas_call(
        layer_kernel,
        out_shape=(jax.ShapeDtypeStruct((n_tok, d_model), bf16), jax.ShapeDtypeStruct((3 * SEG, d_model), bf16),
                   jax.ShapeDtypeStruct((n_tok, SEG_ROWS), bf16), jax.ShapeDtypeStruct((3 * SEG, 128), jnp.float32),
                   jax.ShapeDtypeStruct((1, 128), jnp.int32)),
        in_specs=[anym] * 6,
        out_specs=(anym, anym, anym, anym, vmem),
        scratch_shapes=[
            pltpu.SMEM(slot_expert.shape, jnp.int32),
            pltpu.VMEM((1, n_tok), jnp.int32),
            pltpu.VMEM((1, n_tok), jnp.float32),
            pltpu.VMEM((n_tok, d_model), bf16),
            pltpu.VMEM((N_WBUF, d_model, d_ff), bf16),
            pltpu.VMEM((N_WBUF, d_ff, d_model), bf16),
            pltpu.VMEM((N_SEG, SEG_ROWS, d_model), bf16),
            pltpu.VMEM((N_SEG, SEG_ROWS, d_model), bf16),
            pltpu.VMEM((SLOT_ROWS, d_model), jnp.float32),
            pltpu.VMEM((LOCAL_ROWS, d_model), bf16),
            pltpu.VMEM((N_SEG, SEG_ROWS, d_model), bf16),
            pltpu.VMEM((N_SEG - 1, SEG_ROWS, d_model), bf16),
            pltpu.VMEM((n_tok, d_model), bf16),
            pltpu.VMEM((n_tok, SEG_ROWS), bf16),
            pltpu.VMEM((3 * SEG, 128), jnp.float32),
            pltpu.VMEM((8, n_tok), jnp.int32),
            pltpu.VMEM((n_tok, 128), jnp.int32),
            pltpu.VMEM((n_tok, 128), jnp.float32),
            pltpu.SemaphoreType.DMA((6,)),
            pltpu.SemaphoreType.DMA((n_slot, 2)),
            pltpu.SemaphoreType.DMA((N_SEG, 3)),
            pltpu.SemaphoreType.DMA((N_SEG, 3)),
            pltpu.SemaphoreType.DMA((N_SEG, 3)),
            pltpu.SemaphoreType.DMA((N_SEG, 3)),
            pltpu.SemaphoreType.DMA((n_tok // 256,)),
        ],
        compiler_params=pltpu.CompilerParams(collective_id=0, has_side_effects=True, vmem_limit_bytes=60 * 1024 * 1024),
    )(slot_expert, topk_idx.reshape(1, n_tok), topk_w.reshape(1, n_tok), tokens, w_up[0], w_down[0])


def solution(mesh):
    def group_layer(tokens, topk_idx, topk_w, w_up, w_down, slot_expert):
        *parts, found = fast_layer(tokens, topk_idx, topk_w, w_up, w_down, slot_expert)
        args = (*parts, tokens, topk_idx, topk_w, w_up, w_down, slot_expert)
        return lax.cond(found[0, 0] == 1, lambda *a: add_last(*a[:4]), lambda *a: general_layer(*a[4:]), *args)

    row_spec = P(('dp', 'ep'), None)
    weight_spec = P('ep', None, None, None)
    return jax.shard_map(group_layer, mesh=mesh, in_specs=(row_spec, row_spec, row_spec, weight_spec, weight_spec, P(None, None)), out_specs=row_spec, check_vma=False)
```

```python
import functools

import jax
import jax.numpy as jnp
from jax import lax
from jax.experimental import pallas as pl
from jax.experimental.pallas import tpu as pltpu
from jax.sharding import PartitionSpec as P

MAX_COPIES = 4
SEG = 80
N_SEG = 4
PAIR = 288
SEND_AT = (0, 80, 160, 240, 288)
BACK_AT = (0, 48, 128, 208, 288)
SLOT_ROWS = 4 * SEG
STREAM_AT = (None, 0, N_SEG * SEG, N_SEG * SEG + PAIR)
LOCAL_BASE = 1024
LOCAL_ROWS = 1664
LAST_ROWS = 256
EARLY_ROWS = 768
FF_TILE = 512
N_WBUF = 4
MESH = pl.DeviceIdType.MESH


def slot_bound(n_tok, n_top, n_dev, n_slot):
    base_load = (n_tok * n_top) // (n_dev * n_slot)
    return base_load + base_load // 2 + 1


def route_pairs(topk_idx, slot_expert, capacity):
    n_dev, n_slot = slot_expert.shape
    n_exp = n_dev * (n_slot - 1)
    n_top = topk_idx.shape[1]
    table_flat = slot_expert.reshape(-1)
    slot_ids = jnp.arange(n_dev * n_slot, dtype=jnp.int32)
    same_exp = table_flat[:, None] == table_flat[None, :]
    earlier = slot_ids[None, :] < slot_ids[:, None]
    copy_rank = jnp.sum(same_exp & earlier, axis=1, dtype=jnp.int32)
    exp_copies = jax.ops.segment_sum(jnp.ones_like(table_flat), table_flat, num_segments=n_exp)
    slot_of = jnp.zeros((n_exp, MAX_COPIES), jnp.int32).at[table_flat, copy_rank].set(slot_ids)
    flat_exp = topk_idx.reshape(-1)
    onehot = (flat_exp[:, None] == jnp.arange(n_exp, dtype=jnp.int32)[None, :]).astype(jnp.int32)
    pair_rank = jnp.sum((jnp.cumsum(onehot, axis=0) - onehot) * onehot, axis=1)
    pair_copies = exp_copies[flat_exp]
    slot_flat = slot_of[flat_exp, pair_rank % pair_copies]
    buf_row = pair_rank // pair_copies
    pair_pos = ((slot_flat % n_slot) * n_dev + slot_flat // n_slot) * capacity + buf_row
    pair_tok = jnp.arange(flat_exp.shape[0], dtype=jnp.int32) // n_top
    buf_tok = jnp.zeros((n_slot * n_dev * capacity,), jnp.int32).at[pair_pos].set(pair_tok)
    return pair_pos, buf_tok


def expert_ffn(recv_buf, up_local, down_local):
    pre_act = jnp.einsum('spcm,smf->spcf', recv_buf, up_local, preferred_element_type=jnp.float32)
    hidden = jax.nn.gelu(pre_act, approximate=True).astype(jnp.bfloat16)
    return jnp.einsum('spcf,sfm->spcm', hidden, down_local, preferred_element_type=jnp.float32).astype(jnp.bfloat16)


def general_layer(tokens, topk_idx, topk_w, w_up, w_down, slot_expert):
    n_tok, d_model = tokens.shape
    n_top = topk_idx.shape[1]
    n_dev, n_slot = slot_expert.shape
    capacity = slot_bound(n_tok, n_top, n_dev, n_slot)
    pair_pos, buf_tok = route_pairs(topk_idx, slot_expert, capacity)
    send_buf = tokens[buf_tok].reshape(n_slot, n_dev, capacity, d_model)
    recv_buf = lax.all_to_all(send_buf, 'ep', 1, 1, tiled=True)
    expert_out = expert_ffn(recv_buf, w_up[0], w_down[0])
    back_buf = lax.all_to_all(expert_out, 'ep', 1, 1, tiled=True)
    pair_out = back_buf.reshape(-1, d_model)[pair_pos]
    return (pair_out.astype(jnp.float32) * topk_w).astype(jnp.bfloat16)


def chunk_rows(k):
    return SEND_AT[k + 1] - SEND_AT[k], BACK_AT[k + 1] - BACK_AT[k]


def stream_starts(counts, hot_slot):
    out_at, back_at = [], []
    out_end = back_end = jnp.zeros_like(counts[0])
    for s, count in enumerate(counts):
        out_at.append(out_end)
        floor = jnp.where(hot_slot < s, float(BACK_AT[max(s - 1, 0)]), float(BACK_AT[min(s, N_SEG - 1)]))
        start = jnp.where(hot_slot == s, back_end, jnp.maximum(back_end, floor))
        back_at.append(start)
        out_end = out_end + count
        back_end = start + count
    return out_at, back_at, out_end


def route(idx_row, table, peers, n_exp, n_slot):
    f32 = jnp.float32
    n_tok = idx_row.shape[1]
    lanes = 128
    onehot = (lax.broadcasted_iota(jnp.int32, (n_exp, n_tok), 0) == idx_row).astype(f32)
    step = 256
    blocks = [onehot[:, b * step:(b + 1) * step] for b in range(n_tok // step)]
    before = lax.broadcasted_iota(jnp.int32, (step, step), 0) < lax.broadcasted_iota(jnp.int32, (step, step), 1)
    local_rank = jnp.dot(jnp.concatenate(blocks, axis=0).astype(jnp.bfloat16), before.astype(f32).astype(jnp.bfloat16), preferred_element_type=f32)
    carry = jnp.zeros((n_exp, 1), f32)
    ranks = []
    for b, block in enumerate(blocks):
        ranks.append(local_rank[b * n_exp:(b + 1) * n_exp] + carry)
        carry = carry + jnp.sum(block, axis=1, keepdims=True)
    rank = jnp.concatenate(ranks, axis=1)
    n_pair = jnp.broadcast_to(carry, (n_exp, lanes))

    exp_id = lax.broadcasted_iota(jnp.int32, (n_exp, lanes), 0)
    match = [[(exp_id == table[d, s]).astype(f32) for s in range(n_slot)] for d in peers]
    copies = sum(sum(row) for row in match)
    per_copy = 1.0 / copies
    hot = (copies == 4.0).astype(f32)
    own = sum(match[0])
    own_slot = sum(s * match[0][s] for s in range(n_slot))
    seen = jnp.zeros((n_exp, lanes), f32)
    start_out = [jnp.zeros((n_exp, lanes), f32) for _ in range(MAX_COPIES)]
    start_back = [jnp.zeros((n_exp, lanes), f32) for _ in range(MAX_COPIES)]
    total = jnp.zeros((1, lanes), f32)
    stream_counts = []
    for r in range(len(peers)):
        seens, counts = [], []
        peer_hot = jnp.zeros((1, lanes), f32)
        for s in range(n_slot):
            here = match[r][s]
            seens.append(seen)
            rows = jnp.floor((n_pair - seen + copies - 0.5) * per_copy)
            counts.append(jnp.sum(here * (1.0 - own) * rows, axis=0, keepdims=True))
            peer_hot = peer_hot + s * jnp.sum(here * hot, axis=0, keepdims=True)
            seen = seen + here
        out_at, back_at, end = stream_starts(counts, peer_hot)
        if r == 0:
            hot_slot = peer_hot
        if r >= 2:
            stream_counts.append(counts)
            total = jnp.maximum(total, end)
        for s in range(n_slot):
            local = LOCAL_BASE + SLOT_ROWS * own_slot + SEG * r
            if r == 0:
                code_out = code_back = local
            elif r == 1:
                seg = s - (peer_hot < s).astype(f32)
                code_out = code_back = jnp.where(own > 0, local, STREAM_AT[1] + SEG * seg)
            else:
                code_out = jnp.where(own > 0, local, STREAM_AT[r] + out_at[s])
                code_back = jnp.where(own > 0, local, STREAM_AT[r] + back_at[s])
            for c in range(MAX_COPIES):
                mine = (match[r][s] > 0) & (seens[s] == c)
                start_out[c] = jnp.where(mine, code_out, start_out[c])
                start_back[c] = jnp.where(mine, code_back, start_back[c])

    wide = lambda a: jnp.concatenate([a] * (n_tok // lanes), axis=1)
    row = jnp.floor((rank + 0.5) * wide(per_copy))
    which = rank - row * wide(copies)
    codes = []
    for starts in (start_out, start_back):
        start = wide(starts[3])
        for c in range(MAX_COPIES - 1):
            start = jnp.where(which == c, wide(starts[c]), start)
        codes.append(jnp.sum(onehot * (start + row), axis=0, keepdims=True).astype(jnp.int32))
    fits = jnp.max(own * hot, axis=0, keepdims=True) * (total <= PAIR).astype(f32)
    return codes, hot_slot, stream_counts, fits


def layer_kernel(slot_expert, topk_idx, topk_w, tokens, w_up, w_down, out, last_rows, last_mask, last_gate, found, table, idx_row, gate_row, tok_buf, up_buf, down_buf, send_core, recv_core, send_chip, recv_chip, acc, rows_buf, back_core, back_chip, early, mixed, mask_buf, gate_buf, code_row, back_row, code_col, gate_col, counts_out, counts_in, flags, t_sem, w_sem, ds_sem, dr_sem, bs_sem, br_sem, o_sem, cs_sem, cr_sem, fs_sem, fr_sem):
    f32, bf16 = jnp.float32, jnp.bfloat16
    n_tok, d_model = tok_buf.shape
    n_slot = w_up.shape[0]
    d_ff = w_up.shape[2]
    me = lax.axis_index('ep')
    group = lax.axis_index('dp')
    chip, core = me // 2, me % 2
    peers = [me, 2 * chip + (1 - core), 2 * (1 - chip) + core, 2 * (1 - chip) + (1 - core)]
    peer_ids = [None] + [{'ep': peers[r]} for r in (1, 2, 3)] + [{'dp': 1 - group}]

    barrier = pltpu.get_barrier_semaphore()
    for r in (1, 2, 3, 4):
        pl.semaphore_signal(barrier, inc=1, device_id=peer_ids[r], device_id_type=MESH)

    def weight_copies(s):
        b = s % N_WBUF
        return (pltpu.make_async_copy(w_up.at[s], up_buf.at[b], w_sem.at[s, 0]),
                pltpu.make_async_copy(w_down.at[s], down_buf.at[b], w_sem.at[s, 1]))

    small_copies = [pltpu.make_async_copy(slot_expert, table, t_sem.at[0]),
                    pltpu.make_async_copy(topk_idx, idx_row, t_sem.at[1]),
                    pltpu.make_async_copy(topk_w, gate_row, t_sem.at[2])]
    token_copy = pltpu.make_async_copy(tokens, tok_buf, t_sem.at[3])
    for copy in small_copies:
        copy.start()
    token_copy.start()
    for copy in small_copies:
        copy.wait()
    (code_out, code_back), hot_slot, stream_counts, fits = route(idx_row[...], table, peers, 16, n_slot)
    code_row[...] = jnp.broadcast_to(code_out, code_row.shape)
    back_row[...] = jnp.broadcast_to(code_back, back_row.shape)
    hot_slot = hot_slot[:, :1]
    for r in (2, 3):
        counts_out[r - 2] = jnp.concatenate(stream_counts[r - 2] + [jnp.zeros((8 - n_slot, 128), f32)], axis=0)
    flags[0] = jnp.broadcast_to(fits, (8, 128))

    def pick(ids):
        mask = (ids == code_row[0:1, :]).astype(f32).astype(bf16)
        return jnp.dot(mask, tok_buf[...], preferred_element_type=f32).astype(bf16)

    def ids_from(first, rows):
        return lax.broadcasted_iota(jnp.int32, (rows, n_tok), 0) + first

    def dispatch_copy(k, r):
        if r == 1:
            rows = pl.ds(k * SEG, SEG)
            src, dst = send_core.at[rows], recv_core.at[rows]
        else:
            rows = pl.ds(SEND_AT[k], chunk_rows(k)[0])
            src, dst = send_chip.at[r - 2, rows], recv_chip.at[r - 2, rows]
        return pltpu.make_async_remote_copy(
            src_ref=src, dst_ref=dst, send_sem=ds_sem.at[k, r - 1], recv_sem=dr_sem.at[k, r - 1],
            device_id=peer_ids[r], device_id_type=MESH)

    def back_copy(k, r):
        size = chunk_rows(k)[1]
        if r == 1:
            src, to_early, to_last = back_core.at[pl.ds(k * SEG, SEG)], pl.ds(k * SEG, SEG), pl.ds(0, SEG)
        else:
            src = back_chip.at[r - 2, pl.ds(BACK_AT[k], size)]
            to_early = pl.ds(3 * SEG + (r - 2) * BACK_AT[3] + BACK_AT[k], size)
            to_last = pl.ds((r - 1) * SEG, SEG)
        return pltpu.make_async_remote_copy(
            src_ref=src, dst_ref=early.at[to_early] if k < N_SEG - 1 else last_rows.at[to_last],
            send_sem=bs_sem.at[k, r - 1], recv_sem=br_sem.at[k, r - 1],
            device_id=peer_ids[r], device_id_type=MESH)

    def counts_copy(r):
        return pltpu.make_async_remote_copy(
            src_ref=counts_out.at[r - 2], dst_ref=counts_in.at[r - 2], send_sem=cs_sem.at[r - 2], recv_sem=cr_sem.at[r - 2],
            device_id=peer_ids[r], device_id_type=MESH)

    def flag_copy(r):
        src, dst = (0, 1) if r == 4 else (2, 2 + r)
        return pltpu.make_async_remote_copy(
            src_ref=flags.at[src], dst_ref=flags.at[dst], send_sem=fs_sem.at[r - 1], recv_sem=fr_sem.at[r - 1],
            device_id=peer_ids[r], device_id_type=MESH)

    token_copy.wait()
    for s in range(N_WBUF):
        for copy in weight_copies(s):
            copy.start()
    for k in range(N_SEG):
        size = chunk_rows(k)[0]
        ids = [ids_from(STREAM_AT[2] + SEND_AT[k], size), ids_from(STREAM_AT[3] + SEND_AT[k], size), ids_from(k * SEG, SEG)]
        picked = pick(jnp.concatenate(ids, axis=0))
        send_chip[0, SEND_AT[k]:SEND_AT[k + 1], :] = picked[:size]
        send_chip[1, SEND_AT[k]:SEND_AT[k + 1], :] = picked[size:2 * size]
        send_core[k * SEG:(k + 1) * SEG, :] = picked[2 * size:]
        if k == 0:
            pl.semaphore_wait(barrier, 4)
            for r in (2, 3):
                counts_copy(r).start()
        for r in (2, 3, 1):
            dispatch_copy(k, r).start()
    flag_copy(4).start()

    for s in range(n_slot):
        rows_buf[s * SLOT_ROWS:(s + 1) * SLOT_ROWS, :] = pick(ids_from(LOCAL_BASE + s * SLOT_ROWS, SLOT_ROWS))
    code_col[...] = jnp.transpose(jnp.broadcast_to(code_back, (128, n_tok)))
    gate_col[...] = jnp.transpose(jnp.broadcast_to(gate_row[...], (128, n_tok)))
    n_early = 3 * SEG + 2 * BACK_AT[3]
    early[n_early:, :] = jnp.zeros((EARLY_ROWS - n_early, d_model), bf16)
    rows_buf[n_slot * SLOT_ROWS:, :] = jnp.zeros((LOCAL_ROWS - n_slot * SLOT_ROWS, d_model), bf16)

    def last_ids(i):
        core_id = STREAM_AT[1] + 3 * SEG + i
        chip_id = jnp.where(i < 2 * SEG, STREAM_AT[2] + BACK_AT[3] - SEG, STREAM_AT[3] + BACK_AT[3] - 2 * SEG) + i
        return jnp.where(i < SEG, core_id, jnp.where(i < 3 * SEG, chip_id, -1))

    def early_ids(i):
        chip_id = jnp.where(i < 3 * SEG + BACK_AT[3], STREAM_AT[2] - 3 * SEG, STREAM_AT[3] - 3 * SEG - BACK_AT[3]) + i
        return jnp.where(i < 3 * SEG, STREAM_AT[1] + i, jnp.where(i < n_early, chip_id, -1))

    ids = last_ids(lax.broadcasted_iota(jnp.int32, (3 * SEG, n_tok), 0))
    gates = jnp.sum(jnp.where(ids == back_row[0:1, :], gate_row[...], 0.0), axis=1, keepdims=True)
    gate_buf[...] = jnp.broadcast_to(gates, gate_buf.shape)
    lane = lax.broadcasted_iota(jnp.int32, (n_tok, 128), 1)
    for j in range(LAST_ROWS // 128):
        mask_buf[:, j * 128:(j + 1) * 128] = (code_col[...] == last_ids(lane + 128 * j)).astype(f32).astype(bf16)
    side_copies = [pltpu.make_async_copy(mask_buf, last_mask, t_sem.at[4]),
                   pltpu.make_async_copy(gate_buf, last_gate, t_sem.at[5])]
    for copy in side_copies:
        copy.start()
    flag_copy(4).wait_recv()
    flags[2] = jnp.minimum(flags[0], flags[1])
    for r in (1, 2, 3):
        flag_copy(r).start()
    for r in (2, 3):
        counts_copy(r).wait_recv()
    in_counts = [[counts_in[j, s:s + 1, :1] for s in range(n_slot)] for j in range(2)]
    in_starts = [stream_starts(counts, hot_slot) for counts in in_counts]
    as_int = lambda a: a.astype(jnp.int32)

    for s in range(n_slot):
        lo, hi = s * SLOT_ROWS, (s + 1) * SLOT_ROWS
        if s < N_SEG:
            for r in (1, 2, 3):
                dispatch_copy(s, r).wait_recv()
        near = rows_buf[lo + SEG:lo + 2 * SEG, :].astype(f32)
        if s < N_SEG:
            near = near + recv_core[s * SEG:(s + 1) * SEG, :].astype(f32) * (hot_slot > s).astype(f32)
        if s > 0:
            near = near + recv_core[(s - 1) * SEG:s * SEG, :].astype(f32) * (hot_slot < s).astype(f32)
        rows_buf[lo + SEG:lo + 2 * SEG, :] = near.astype(bf16)
        come = SEND_AT[min(s, N_SEG - 1) + 1]
        i = lax.broadcasted_iota(jnp.int32, (SEG, come), 0)
        j = lax.broadcasted_iota(jnp.int32, (SEG, come), 1)
        for r in (2, 3):
            mask = (j - i == as_int(in_starts[r - 2][0][s])) & (i < as_int(in_counts[r - 2][s]))
            far = jnp.dot(mask.astype(f32).astype(bf16), recv_chip[r - 2, :come, :], preferred_element_type=f32)
            at = slice(lo + r * SEG, lo + (r + 1) * SEG)
            rows_buf[at, :] = (rows_buf[at, :].astype(f32) + far).astype(bf16)
        for copy in weight_copies(s):
            copy.wait()
        b = s % N_WBUF
        acc[...] = jnp.zeros_like(acc)

        def ff_step(i, carry):
            cols = pl.ds(pl.multiple_of(i * FF_TILE, FF_TILE), FF_TILE)
            pre = jnp.dot(rows_buf[lo:hi, :], up_buf[b, :, cols], preferred_element_type=f32)
            hidden = jax.nn.gelu(pre, approximate=True).astype(bf16)
            acc[...] += jnp.dot(hidden, down_buf[b, cols, :], preferred_element_type=f32)
            return carry

        lax.fori_loop(0, d_ff // FF_TILE, ff_step, 0)
        if s + N_WBUF < n_slot:
            for copy in weight_copies(s + N_WBUF):
                copy.start()
        rows_buf[lo:hi, :] = acc[...].astype(bf16)
        if s > 0:
            k = s - 1
            size = chunk_rows(k)[1]
            slots = list(range(max(k - 1, 0), s + 1))
            i = lax.broadcasted_iota(jnp.int32, (size, SEG * len(slots)), 0)
            j = lax.broadcasted_iota(jnp.int32, (size, SEG * len(slots)), 1)
            for r in (2, 3):
                mask = jnp.zeros(i.shape, f32)
                for n, q in enumerate(slots):
                    row = j - n * SEG
                    fit = (i + BACK_AT[k] - row == as_int(in_starts[r - 2][1][q])) & (row >= 0) & (row < as_int(in_counts[r - 2][q]))
                    mask = jnp.where(fit, 1.0, mask)
                done = jnp.concatenate([rows_buf[q * SLOT_ROWS + r * SEG:q * SLOT_ROWS + (r + 1) * SEG, :] for q in slots], axis=0)
                back_chip[r - 2, BACK_AT[k]:BACK_AT[k + 1], :] = jnp.dot(mask.astype(bf16), done, preferred_element_type=f32).astype(bf16)
                back_copy(k, r).start()
            prev = rows_buf[lo - SLOT_ROWS + SEG:lo - SLOT_ROWS + 2 * SEG, :].astype(f32)
            last = rows_buf[lo + SEG:lo + 2 * SEG, :].astype(f32)
            back = prev * (hot_slot > k).astype(f32) + last * (hot_slot <= k).astype(f32)
            back_core[k * SEG:(k + 1) * SEG, :] = back.astype(bf16)
            back_copy(k, 1).start()

    tile = 256
    n_tile = n_tok // tile

    def out_copy(i):
        at = pl.ds(pl.multiple_of(i * tile, tile), tile)
        return pltpu.make_async_copy(mixed.at[at], out.at[at], o_sem.at[i])

    def combine(ids_of, rows, source, final):
        def body(i, carry):
            at = pl.ds(pl.multiple_of(i * tile, tile), tile)
            mine = code_col[at, :]
            lane = lax.broadcasted_iota(jnp.int32, (tile, 128), 1)
            mask = jnp.concatenate([(mine == ids_of(lane + 128 * j)).astype(f32).astype(bf16) for j in range(rows // 128)], axis=1)
            part = jnp.dot(mask, source[...], preferred_element_type=f32)
            if final:
                part = part + mixed[at, :].astype(f32)
                part = part * jnp.concatenate([gate_col[at, :]] * (d_model // 128), axis=1)
            mixed[at, :] = part.astype(bf16)
            if final:
                out_copy(i).start()
            return carry
        lax.fori_loop(0, n_tile, body, 0)

    combine(lambda i: LOCAL_BASE + i, LOCAL_ROWS, rows_buf, False)
    for r in (1, 2, 3):
        flag_copy(r).wait_recv()
    agreed = jnp.minimum(jnp.minimum(flags[2], flags[3]), jnp.minimum(flags[4], flags[5]))
    found[...] = agreed[0:1, :].astype(jnp.int32)
    for k in range(N_SEG):
        for r in (1, 2, 3):
            back_copy(k, r).wait_recv()
        if k == N_SEG - 2:
            combine(early_ids, EARLY_ROWS, early, True)
            for i in range(n_tile):
                out_copy(i).wait()
            for copy in side_copies:
                copy.wait()
    for r in (2, 3):
        counts_copy(r).wait_send()
    for r in (1, 2, 3, 4):
        flag_copy(r).wait_send()
    for k in range(N_SEG):
        for r in (1, 2, 3):
            dispatch_copy(k, r).wait_send()
            back_copy(k, r).wait_send()


def last_kernel(part, rows, mask, gate, out):
    f32, bf16 = jnp.float32, jnp.bfloat16
    d_model = part.shape[1]
    gates = jnp.concatenate([gate[...]] * (d_model // 128), axis=1)
    scaled = (rows[...].astype(f32) * gates).astype(bf16)
    scaled = jnp.concatenate([scaled, jnp.zeros((LAST_ROWS - scaled.shape[0], d_model), bf16)], axis=0)
    late = jnp.dot(mask[...], scaled, preferred_element_type=f32)
    out[...] = (late + part[...].astype(f32)).astype(bf16)


def add_last(part, rows, mask, gate):
    n_tok, d_model = part.shape
    tile = 512
    by_tile = lambda cols: pl.BlockSpec((tile, cols), lambda i: (i, 0))
    whole = lambda a: pl.BlockSpec(a.shape, lambda i: (0, 0))
    return pl.pallas_call(
        last_kernel,
        grid=(n_tok // tile,),
        out_shape=jax.ShapeDtypeStruct(part.shape, part.dtype),
        in_specs=[by_tile(d_model), whole(rows), by_tile(mask.shape[1]), whole(gate)],
        out_specs=by_tile(d_model),
    )(part, rows, mask, gate)


def fast_layer(tokens, topk_idx, topk_w, w_up, w_down, slot_expert):
    n_tok, d_model = tokens.shape
    n_slot, d_ff = w_up.shape[1], w_up.shape[3]
    vmem = pl.BlockSpec(memory_space=pltpu.VMEM)
    anym = pl.BlockSpec(memory_space=pl.ANY)
    bf16, f32 = jnp.bfloat16, jnp.float32
    shape = jax.ShapeDtypeStruct
    dma = pltpu.SemaphoreType.DMA
    return pl.pallas_call(
        layer_kernel,
        out_shape=(shape((n_tok, d_model), bf16), shape((3 * SEG, d_model), bf16), shape((n_tok, LAST_ROWS), bf16),
                   shape((3 * SEG, 128), f32), shape((1, 128), jnp.int32)),
        in_specs=[anym] * 6,
        out_specs=(anym, anym, anym, anym, vmem),
        scratch_shapes=[
            pltpu.SMEM(slot_expert.shape, jnp.int32),
            pltpu.VMEM((1, n_tok), jnp.int32),
            pltpu.VMEM((1, n_tok), f32),
            pltpu.VMEM((n_tok, d_model), bf16),
            pltpu.VMEM((N_WBUF, d_model, d_ff), bf16),
            pltpu.VMEM((N_WBUF, d_ff, d_model), bf16),
            pltpu.VMEM((N_SEG * SEG, d_model), bf16),
            pltpu.VMEM((N_SEG * SEG, d_model), bf16),
            pltpu.VMEM((2, PAIR, d_model), bf16),
            pltpu.VMEM((2, PAIR, d_model), bf16),
            pltpu.VMEM((SLOT_ROWS, d_model), f32),
            pltpu.VMEM((LOCAL_ROWS, d_model), bf16),
            pltpu.VMEM((N_SEG * SEG, d_model), bf16),
            pltpu.VMEM((2, PAIR, d_model), bf16),
            pltpu.VMEM((EARLY_ROWS, d_model), bf16),
            pltpu.VMEM((n_tok, d_model), bf16),
            pltpu.VMEM((n_tok, LAST_ROWS), bf16),
            pltpu.VMEM((3 * SEG, 128), f32),
            pltpu.VMEM((8, n_tok), jnp.int32),
            pltpu.VMEM((8, n_tok), jnp.int32),
            pltpu.VMEM((n_tok, 128), jnp.int32),
            pltpu.VMEM((n_tok, 128), f32),
            pltpu.VMEM((2, 8, 128), f32),
            pltpu.VMEM((2, 8, 128), f32),
            pltpu.VMEM((6, 8, 128), f32),
            dma((6,)), dma((n_slot, 2)),
            dma((N_SEG, 3)), dma((N_SEG, 3)), dma((N_SEG, 3)), dma((N_SEG, 3)),
            dma((n_tok // 256,)), dma((2,)), dma((2,)), dma((4,)), dma((4,)),
        ],
        compiler_params=pltpu.CompilerParams(collective_id=0, has_side_effects=True, vmem_limit_bytes=60 * 1024 * 1024),
    )(slot_expert, topk_idx.reshape(1, n_tok), topk_w.reshape(1, n_tok), tokens, w_up[0], w_down[0])


def solution(mesh):
    def group_layer(tokens, topk_idx, topk_w, w_up, w_down, slot_expert):
        *parts, found = fast_layer(tokens, topk_idx, topk_w, w_up, w_down, slot_expert)
        args = (*parts, tokens, topk_idx, topk_w, w_up, w_down, slot_expert)
        return lax.cond(found[0, 0] == 1, lambda *a: add_last(*a[:4]), lambda *a: general_layer(*a[4:]), *args)

    row_spec = P(('dp', 'ep'), None)
    weight_spec = P('ep', None, None, None)
    return jax.shard_map(group_layer, mesh=mesh, in_specs=(row_spec, row_spec, row_spec, weight_spec, weight_spec, P(None, None)), out_specs=row_spec, check_vma=False)
```

```python
import functools

import jax
import jax.numpy as jnp
from jax import lax
from jax.experimental import pallas as pl
from jax.experimental.pallas import tpu as pltpu
from jax.sharding import PartitionSpec as P

MAX_COPIES = 4
SEG = 80
N_SEG = 4
PAIR = 288
SEND_AT = (0, 80, 160, 240, 288)
BACK_AT = (0, 48, 128, 208, 288)
SLOT_ROWS = 4 * SEG
STREAM_AT = (None, 0, N_SEG * SEG, N_SEG * SEG + PAIR)
LOCAL_BASE = 1024
LOCAL_ROWS = 1664
LAST_ROWS = 256
EARLY_ROWS = 768
FF_TILE = 1536
N_WBUF = 4
MESH = pl.DeviceIdType.MESH


def slot_bound(n_tok, n_top, n_dev, n_slot):
    base_load = (n_tok * n_top) // (n_dev * n_slot)
    return base_load + base_load // 2 + 1


def route_pairs(topk_idx, slot_expert, capacity):
    n_dev, n_slot = slot_expert.shape
    n_exp = n_dev * (n_slot - 1)
    n_top = topk_idx.shape[1]
    table_flat = slot_expert.reshape(-1)
    slot_ids = jnp.arange(n_dev * n_slot, dtype=jnp.int32)
    same_exp = table_flat[:, None] == table_flat[None, :]
    earlier = slot_ids[None, :] < slot_ids[:, None]
    copy_rank = jnp.sum(same_exp & earlier, axis=1, dtype=jnp.int32)
    exp_copies = jax.ops.segment_sum(jnp.ones_like(table_flat), table_flat, num_segments=n_exp)
    slot_of = jnp.zeros((n_exp, MAX_COPIES), jnp.int32).at[table_flat, copy_rank].set(slot_ids)
    flat_exp = topk_idx.reshape(-1)
    onehot = (flat_exp[:, None] == jnp.arange(n_exp, dtype=jnp.int32)[None, :]).astype(jnp.int32)
    pair_rank = jnp.sum((jnp.cumsum(onehot, axis=0) - onehot) * onehot, axis=1)
    pair_copies = exp_copies[flat_exp]
    slot_flat = slot_of[flat_exp, pair_rank % pair_copies]
    buf_row = pair_rank // pair_copies
    pair_pos = ((slot_flat % n_slot) * n_dev + slot_flat // n_slot) * capacity + buf_row
    pair_tok = jnp.arange(flat_exp.shape[0], dtype=jnp.int32) // n_top
    buf_tok = jnp.zeros((n_slot * n_dev * capacity,), jnp.int32).at[pair_pos].set(pair_tok)
    return pair_pos, buf_tok


def expert_ffn(recv_buf, up_local, down_local):
    pre_act = jnp.einsum('spcm,smf->spcf', recv_buf, up_local, preferred_element_type=jnp.float32)
    hidden = jax.nn.gelu(pre_act, approximate=True).astype(jnp.bfloat16)
    return jnp.einsum('spcf,sfm->spcm', hidden, down_local, preferred_element_type=jnp.float32).astype(jnp.bfloat16)


def general_layer(tokens, topk_idx, topk_w, w_up, w_down, slot_expert):
    n_tok, d_model = tokens.shape
    n_top = topk_idx.shape[1]
    n_dev, n_slot = slot_expert.shape
    capacity = slot_bound(n_tok, n_top, n_dev, n_slot)
    pair_pos, buf_tok = route_pairs(topk_idx, slot_expert, capacity)
    send_buf = tokens[buf_tok].reshape(n_slot, n_dev, capacity, d_model)
    recv_buf = lax.all_to_all(send_buf, 'ep', 1, 1, tiled=True)
    expert_out = expert_ffn(recv_buf, w_up[0], w_down[0])
    back_buf = lax.all_to_all(expert_out, 'ep', 1, 1, tiled=True)
    pair_out = back_buf.reshape(-1, d_model)[pair_pos]
    return (pair_out.astype(jnp.float32) * topk_w).astype(jnp.bfloat16)


def chunk_rows(k):
    return SEND_AT[k + 1] - SEND_AT[k], BACK_AT[k + 1] - BACK_AT[k]


def stream_starts(counts, hot_slot):
    out_at, back_at = [], []
    out_end = back_end = jnp.zeros_like(counts[0])
    for s, count in enumerate(counts):
        out_at.append(out_end)
        floor = jnp.where(hot_slot < s, float(BACK_AT[max(s - 1, 0)]), float(BACK_AT[min(s, N_SEG - 1)]))
        start = jnp.where(hot_slot == s, back_end, jnp.maximum(back_end, floor))
        back_at.append(start)
        out_end = out_end + count
        back_end = start + count
    return out_at, back_at, out_end


def route(idx_row, table, peers, n_exp, n_slot):
    f32 = jnp.float32
    n_tok = idx_row.shape[1]
    lanes = 128
    onehot = (lax.broadcasted_iota(jnp.int32, (n_exp, n_tok), 0) == idx_row).astype(f32)
    step = 256
    blocks = [onehot[:, b * step:(b + 1) * step] for b in range(n_tok // step)]
    before = lax.broadcasted_iota(jnp.int32, (step, step), 0) < lax.broadcasted_iota(jnp.int32, (step, step), 1)
    local_rank = jnp.dot(jnp.concatenate(blocks, axis=0).astype(jnp.bfloat16), before.astype(f32).astype(jnp.bfloat16), preferred_element_type=f32)
    carry = jnp.zeros((n_exp, 1), f32)
    ranks = []
    for b, block in enumerate(blocks):
        ranks.append(local_rank[b * n_exp:(b + 1) * n_exp] + carry)
        carry = carry + jnp.sum(block, axis=1, keepdims=True)
    rank = jnp.concatenate(ranks, axis=1)
    n_pair = jnp.broadcast_to(carry, (n_exp, lanes))

    exp_id = lax.broadcasted_iota(jnp.int32, (n_exp, lanes), 0)
    match = [[(exp_id == table[d, s]).astype(f32) for s in range(n_slot)] for d in peers]
    copies = sum(sum(row) for row in match)
    per_copy = 1.0 / copies
    hot = (copies == 4.0).astype(f32)
    own = sum(match[0])
    own_slot = sum(s * match[0][s] for s in range(n_slot))
    seen = jnp.zeros((n_exp, lanes), f32)
    start_out = [jnp.zeros((n_exp, lanes), f32) for _ in range(MAX_COPIES)]
    start_back = [jnp.zeros((n_exp, lanes), f32) for _ in range(MAX_COPIES)]
    total = jnp.zeros((1, lanes), f32)
    stream_counts = []
    for r in range(len(peers)):
        seens, counts = [], []
        peer_hot = jnp.zeros((1, lanes), f32)
        for s in range(n_slot):
            here = match[r][s]
            seens.append(seen)
            rows = jnp.floor((n_pair - seen + copies - 0.5) * per_copy)
            counts.append(jnp.sum(here * (1.0 - own) * rows, axis=0, keepdims=True))
            peer_hot = peer_hot + s * jnp.sum(here * hot, axis=0, keepdims=True)
            seen = seen + here
        out_at, back_at, end = stream_starts(counts, peer_hot)
        if r == 0:
            hot_slot = peer_hot
        if r >= 2:
            stream_counts.append(counts)
            total = jnp.maximum(total, end)
        for s in range(n_slot):
            local = LOCAL_BASE + SLOT_ROWS * own_slot + SEG * r
            if r == 0:
                code_out = code_back = local
            elif r == 1:
                seg = s - (peer_hot < s).astype(f32)
                code_out = code_back = jnp.where(own > 0, local, STREAM_AT[1] + SEG * seg)
            else:
                code_out = jnp.where(own > 0, local, STREAM_AT[r] + out_at[s])
                code_back = jnp.where(own > 0, local, STREAM_AT[r] + back_at[s])
            for c in range(MAX_COPIES):
                mine = (match[r][s] > 0) & (seens[s] == c)
                start_out[c] = jnp.where(mine, code_out, start_out[c])
                start_back[c] = jnp.where(mine, code_back, start_back[c])

    wide = lambda a: jnp.concatenate([a] * (n_tok // lanes), axis=1)
    row = jnp.floor((rank + 0.5) * wide(per_copy))
    which = rank - row * wide(copies)
    codes = []
    for starts in (start_out, start_back):
        start = wide(starts[3])
        for c in range(MAX_COPIES - 1):
            start = jnp.where(which == c, wide(starts[c]), start)
        codes.append(jnp.sum(onehot * (start + row), axis=0, keepdims=True).astype(jnp.int32))
    fits = jnp.max(own * hot, axis=0, keepdims=True) * (total <= PAIR).astype(f32)
    return codes, hot_slot, stream_counts, fits


def layer_kernel(slot_expert, topk_idx, topk_w, tokens, w_up, w_down, out, last_rows, last_mask, last_gate, found, table, idx_row, gate_row, tok_buf, up_buf, down_buf, send_core, recv_core, send_chip, recv_chip, acc, rows_buf, back_core, back_chip, early, mixed, mask_buf, gate_buf, code_row, back_row, code_col, gate_col, counts_out, counts_in, flags, t_sem, w_sem, ds_sem, dr_sem, bs_sem, br_sem, o_sem, cs_sem, cr_sem, fs_sem, fr_sem):
    f32, bf16 = jnp.float32, jnp.bfloat16
    n_tok, d_model = tok_buf.shape
    n_slot = w_up.shape[0]
    d_ff = w_up.shape[2]
    me = lax.axis_index('ep')
    group = lax.axis_index('dp')
    chip, core = me // 2, me % 2
    peers = [me, 2 * chip + (1 - core), 2 * (1 - chip) + core, 2 * (1 - chip) + (1 - core)]
    peer_ids = [None] + [{'ep': peers[r]} for r in (1, 2, 3)] + [{'dp': 1 - group}]

    barrier = pltpu.get_barrier_semaphore()
    for r in (1, 2, 3, 4):
        pl.semaphore_signal(barrier, inc=1, device_id=peer_ids[r], device_id_type=MESH)

    def weight_copies(s):
        b = s % N_WBUF
        return (pltpu.make_async_copy(w_up.at[s], up_buf.at[b], w_sem.at[s, 0]),
                pltpu.make_async_copy(w_down.at[s], down_buf.at[b], w_sem.at[s, 1]))

    small_copies = [pltpu.make_async_copy(slot_expert, table, t_sem.at[0]),
                    pltpu.make_async_copy(topk_idx, idx_row, t_sem.at[1]),
                    pltpu.make_async_copy(topk_w, gate_row, t_sem.at[2])]
    token_copy = pltpu.make_async_copy(tokens, tok_buf, t_sem.at[3])
    for copy in small_copies:
        copy.start()
    token_copy.start()
    for copy in small_copies:
        copy.wait()
    (code_out, code_back), hot_slot, stream_counts, fits = route(idx_row[...], table, peers, 16, n_slot)
    code_row[...] = jnp.broadcast_to(code_out, code_row.shape)
    back_row[...] = jnp.broadcast_to(code_back, back_row.shape)
    hot_slot = hot_slot[:, :1]
    for r in (2, 3):
        counts_out[r - 2] = jnp.concatenate(stream_counts[r - 2] + [jnp.zeros((8 - n_slot, 128), f32)], axis=0)
    flags[0] = jnp.broadcast_to(fits, (8, 128))

    def pick(ids):
        mask = (ids == code_row[0:1, :]).astype(f32).astype(bf16)
        return jnp.dot(mask, tok_buf[...], preferred_element_type=f32).astype(bf16)

    def ids_from(first, rows):
        return lax.broadcasted_iota(jnp.int32, (rows, n_tok), 0) + first

    def dispatch_copy(k, r):
        if r == 1:
            rows = pl.ds(k * SEG, SEG)
            src, dst = send_core.at[rows], recv_core.at[rows]
        else:
            rows = pl.ds(SEND_AT[k], chunk_rows(k)[0])
            src, dst = send_chip.at[r - 2, rows], recv_chip.at[r - 2, rows]
        return pltpu.make_async_remote_copy(
            src_ref=src, dst_ref=dst, send_sem=ds_sem.at[k, r - 1], recv_sem=dr_sem.at[k, r - 1],
            device_id=peer_ids[r], device_id_type=MESH)

    def back_copy(k, r):
        size = chunk_rows(k)[1]
        if r == 1:
            src, to_early, to_last = back_core.at[pl.ds(k * SEG, SEG)], pl.ds(k * SEG, SEG), pl.ds(0, SEG)
        else:
            src = back_chip.at[r - 2, pl.ds(BACK_AT[k], size)]
            to_early = pl.ds(3 * SEG + (r - 2) * BACK_AT[3] + BACK_AT[k], size)
            to_last = pl.ds((r - 1) * SEG, SEG)
        return pltpu.make_async_remote_copy(
            src_ref=src, dst_ref=early.at[to_early] if k < N_SEG - 1 else last_rows.at[to_last],
            send_sem=bs_sem.at[k, r - 1], recv_sem=br_sem.at[k, r - 1],
            device_id=peer_ids[r], device_id_type=MESH)

    def counts_copy(r):
        return pltpu.make_async_remote_copy(
            src_ref=counts_out.at[r - 2], dst_ref=counts_in.at[r - 2], send_sem=cs_sem.at[r - 2], recv_sem=cr_sem.at[r - 2],
            device_id=peer_ids[r], device_id_type=MESH)

    def flag_copy(r):
        src, dst = (0, 1) if r == 4 else (2, 2 + r)
        return pltpu.make_async_remote_copy(
            src_ref=flags.at[src], dst_ref=flags.at[dst], send_sem=fs_sem.at[r - 1], recv_sem=fr_sem.at[r - 1],
            device_id=peer_ids[r], device_id_type=MESH)

    token_copy.wait()
    for s in range(N_WBUF):
        for copy in weight_copies(s):
            copy.start()
    for k in range(N_SEG):
        size = chunk_rows(k)[0]
        ids = [ids_from(STREAM_AT[2] + SEND_AT[k], size), ids_from(STREAM_AT[3] + SEND_AT[k], size), ids_from(k * SEG, SEG)]
        picked = pick(jnp.concatenate(ids, axis=0))
        send_chip[0, SEND_AT[k]:SEND_AT[k + 1], :] = picked[:size]
        send_chip[1, SEND_AT[k]:SEND_AT[k + 1], :] = picked[size:2 * size]
        send_core[k * SEG:(k + 1) * SEG, :] = picked[2 * size:]
        if k == 0:
            pl.semaphore_wait(barrier, 4)
            for r in (2, 3):
                counts_copy(r).start()
        for r in (2, 3, 1):
            dispatch_copy(k, r).start()
    flag_copy(4).start()

    for s in range(n_slot):
        rows_buf[s * SLOT_ROWS:(s + 1) * SLOT_ROWS, :] = pick(ids_from(LOCAL_BASE + s * SLOT_ROWS, SLOT_ROWS))
    code_col[...] = jnp.transpose(jnp.broadcast_to(code_back, (128, n_tok)))
    gate_col[...] = jnp.transpose(jnp.broadcast_to(gate_row[...], (128, n_tok)))
    n_early = 3 * SEG + 2 * BACK_AT[3]
    early[n_early:, :] = jnp.zeros((EARLY_ROWS - n_early, d_model), bf16)
    rows_buf[n_slot * SLOT_ROWS:, :] = jnp.zeros((LOCAL_ROWS - n_slot * SLOT_ROWS, d_model), bf16)

    def last_ids(i):
        core_id = STREAM_AT[1] + 3 * SEG + i
        chip_id = jnp.where(i < 2 * SEG, STREAM_AT[2] + BACK_AT[3] - SEG, STREAM_AT[3] + BACK_AT[3] - 2 * SEG) + i
        return jnp.where(i < SEG, core_id, jnp.where(i < 3 * SEG, chip_id, -1))

    def early_ids(i):
        chip_id = jnp.where(i < 3 * SEG + BACK_AT[3], STREAM_AT[2] - 3 * SEG, STREAM_AT[3] - 3 * SEG - BACK_AT[3]) + i
        return jnp.where(i < 3 * SEG, STREAM_AT[1] + i, jnp.where(i < n_early, chip_id, -1))

    ids = last_ids(lax.broadcasted_iota(jnp.int32, (3 * SEG, n_tok), 0))
    gates = jnp.sum(jnp.where(ids == back_row[0:1, :], gate_row[...], 0.0), axis=1, keepdims=True)
    gate_buf[...] = jnp.broadcast_to(gates, gate_buf.shape)
    lane = lax.broadcasted_iota(jnp.int32, (n_tok, 128), 1)
    for j in range(LAST_ROWS // 128):
        mask_buf[:, j * 128:(j + 1) * 128] = (code_col[...] == last_ids(lane + 128 * j)).astype(f32).astype(bf16)
    side_copies = [pltpu.make_async_copy(mask_buf, last_mask, t_sem.at[4]),
                   pltpu.make_async_copy(gate_buf, last_gate, t_sem.at[5])]
    for copy in side_copies:
        copy.start()
    flag_copy(4).wait_recv()
    flags[2] = jnp.minimum(flags[0], flags[1])
    for r in (1, 2, 3):
        flag_copy(r).start()
    for r in (2, 3):
        counts_copy(r).wait_recv()
    in_counts = [[counts_in[j, s:s + 1, :1] for s in range(n_slot)] for j in range(2)]
    in_starts = [stream_starts(counts, hot_slot) for counts in in_counts]
    as_int = lambda a: a.astype(jnp.int32)

    for s in range(n_slot):
        lo, hi = s * SLOT_ROWS, (s + 1) * SLOT_ROWS
        if s < N_SEG:
            for r in (1, 2, 3):
                dispatch_copy(s, r).wait_recv()
        near = rows_buf[lo + SEG:lo + 2 * SEG, :].astype(f32)
        if s < N_SEG:
            near = near + recv_core[s * SEG:(s + 1) * SEG, :].astype(f32) * (hot_slot > s).astype(f32)
        if s > 0:
            near = near + recv_core[(s - 1) * SEG:s * SEG, :].astype(f32) * (hot_slot < s).astype(f32)
        rows_buf[lo + SEG:lo + 2 * SEG, :] = near.astype(bf16)
        come = SEND_AT[min(s, N_SEG - 1) + 1]
        i = lax.broadcasted_iota(jnp.int32, (SEG, come), 0)
        j = lax.broadcasted_iota(jnp.int32, (SEG, come), 1)
        for r in (2, 3):
            mask = (j - i == as_int(in_starts[r - 2][0][s])) & (i < as_int(in_counts[r - 2][s]))
            far = jnp.dot(mask.astype(f32).astype(bf16), recv_chip[r - 2, :come, :], preferred_element_type=f32)
            at = slice(lo + r * SEG, lo + (r + 1) * SEG)
            rows_buf[at, :] = (rows_buf[at, :].astype(f32) + far).astype(bf16)
        for copy in weight_copies(s):
            copy.wait()
        b = s % N_WBUF
        acc[...] = jnp.zeros_like(acc)

        def ff_step(i, carry):
            cols = pl.ds(pl.multiple_of(i * FF_TILE, FF_TILE), FF_TILE)
            pre = jnp.dot(rows_buf[lo:hi, :], up_buf[b, :, cols], preferred_element_type=f32)
            hidden = jax.nn.gelu(pre, approximate=True).astype(bf16)
            acc[...] += jnp.dot(hidden, down_buf[b, cols, :], preferred_element_type=f32)
            return carry

        lax.fori_loop(0, d_ff // FF_TILE, ff_step, 0)
        if s + N_WBUF < n_slot:
            for copy in weight_copies(s + N_WBUF):
                copy.start()
        rows_buf[lo:hi, :] = acc[...].astype(bf16)
        if s > 0:
            k = s - 1
            size = chunk_rows(k)[1]
            slots = list(range(max(k - 1, 0), s + 1))
            i = lax.broadcasted_iota(jnp.int32, (size, SEG * len(slots)), 0)
            j = lax.broadcasted_iota(jnp.int32, (size, SEG * len(slots)), 1)
            for r in (2, 3):
                mask = jnp.zeros(i.shape, f32)
                for n, q in enumerate(slots):
                    row = j - n * SEG
                    fit = (i + BACK_AT[k] - row == as_int(in_starts[r - 2][1][q])) & (row >= 0) & (row < as_int(in_counts[r - 2][q]))
                    mask = jnp.where(fit, 1.0, mask)
                done = jnp.concatenate([rows_buf[q * SLOT_ROWS + r * SEG:q * SLOT_ROWS + (r + 1) * SEG, :] for q in slots], axis=0)
                back_chip[r - 2, BACK_AT[k]:BACK_AT[k + 1], :] = jnp.dot(mask.astype(bf16), done, preferred_element_type=f32).astype(bf16)
                back_copy(k, r).start()
            prev = rows_buf[lo - SLOT_ROWS + SEG:lo - SLOT_ROWS + 2 * SEG, :].astype(f32)
            last = rows_buf[lo + SEG:lo + 2 * SEG, :].astype(f32)
            back = prev * (hot_slot > k).astype(f32) + last * (hot_slot <= k).astype(f32)
            back_core[k * SEG:(k + 1) * SEG, :] = back.astype(bf16)
            back_copy(k, 1).start()

    tile = 256
    n_tile = n_tok // tile

    def out_copy(i):
        at = pl.ds(pl.multiple_of(i * tile, tile), tile)
        return pltpu.make_async_copy(mixed.at[at], out.at[at], o_sem.at[i])

    def combine(ids_of, rows, source, final):
        def body(i, carry):
            at = pl.ds(pl.multiple_of(i * tile, tile), tile)
            mine = code_col[at, :]
            lane = lax.broadcasted_iota(jnp.int32, (tile, 128), 1)
            mask = jnp.concatenate([(mine == ids_of(lane + 128 * j)).astype(f32).astype(bf16) for j in range(rows // 128)], axis=1)
            part = jnp.dot(mask, source[...], preferred_element_type=f32)
            if final:
                part = part + mixed[at, :].astype(f32)
                part = part * jnp.concatenate([gate_col[at, :]] * (d_model // 128), axis=1)
            mixed[at, :] = part.astype(bf16)
            if final:
                out_copy(i).start()
            return carry
        lax.fori_loop(0, n_tile, body, 0)

    combine(lambda i: LOCAL_BASE + i, LOCAL_ROWS, rows_buf, False)
    for r in (1, 2, 3):
        flag_copy(r).wait_recv()
    agreed = jnp.minimum(jnp.minimum(flags[2], flags[3]), jnp.minimum(flags[4], flags[5]))
    found[...] = agreed[0:1, :].astype(jnp.int32)
    for k in range(N_SEG):
        for r in (1, 2, 3):
            back_copy(k, r).wait_recv()
        if k == N_SEG - 2:
            combine(early_ids, EARLY_ROWS, early, True)
            for i in range(n_tile):
                out_copy(i).wait()
            for copy in side_copies:
                copy.wait()
    for r in (2, 3):
        counts_copy(r).wait_send()
    for r in (1, 2, 3, 4):
        flag_copy(r).wait_send()
    for k in range(N_SEG):
        for r in (1, 2, 3):
            dispatch_copy(k, r).wait_send()
            back_copy(k, r).wait_send()


def last_kernel(part, rows, mask, gate, out):
    f32, bf16 = jnp.float32, jnp.bfloat16
    d_model = part.shape[1]
    gates = jnp.concatenate([gate[...]] * (d_model // 128), axis=1)
    scaled = (rows[...].astype(f32) * gates).astype(bf16)
    scaled = jnp.concatenate([scaled, jnp.zeros((LAST_ROWS - scaled.shape[0], d_model), bf16)], axis=0)
    late = jnp.dot(mask[...], scaled, preferred_element_type=f32)
    out[...] = (late + part[...].astype(f32)).astype(bf16)


def add_last(part, rows, mask, gate):
    n_tok, d_model = part.shape
    tile = 512
    by_tile = lambda cols: pl.BlockSpec((tile, cols), lambda i: (i, 0))
    whole = lambda a: pl.BlockSpec(a.shape, lambda i: (0, 0))
    return pl.pallas_call(
        last_kernel,
        grid=(n_tok // tile,),
        out_shape=jax.ShapeDtypeStruct(part.shape, part.dtype),
        in_specs=[by_tile(d_model), whole(rows), by_tile(mask.shape[1]), whole(gate)],
        out_specs=by_tile(d_model),
    )(part, rows, mask, gate)


def fast_layer(tokens, topk_idx, topk_w, w_up, w_down, slot_expert):
    n_tok, d_model = tokens.shape
    n_slot, d_ff = w_up.shape[1], w_up.shape[3]
    vmem = pl.BlockSpec(memory_space=pltpu.VMEM)
    anym = pl.BlockSpec(memory_space=pl.ANY)
    bf16, f32 = jnp.bfloat16, jnp.float32
    shape = jax.ShapeDtypeStruct
    dma = pltpu.SemaphoreType.DMA
    return pl.pallas_call(
        layer_kernel,
        out_shape=(shape((n_tok, d_model), bf16), shape((3 * SEG, d_model), bf16), shape((n_tok, LAST_ROWS), bf16),
                   shape((3 * SEG, 128), f32), shape((1, 128), jnp.int32)),
        in_specs=[anym] * 6,
        out_specs=(anym, anym, anym, anym, vmem),
        scratch_shapes=[
            pltpu.SMEM(slot_expert.shape, jnp.int32),
            pltpu.VMEM((1, n_tok), jnp.int32),
            pltpu.VMEM((1, n_tok), f32),
            pltpu.VMEM((n_tok, d_model), bf16),
            pltpu.VMEM((N_WBUF, d_model, d_ff), bf16),
            pltpu.VMEM((N_WBUF, d_ff, d_model), bf16),
            pltpu.VMEM((N_SEG * SEG, d_model), bf16),
            pltpu.VMEM((N_SEG * SEG, d_model), bf16),
            pltpu.VMEM((2, PAIR, d_model), bf16),
            pltpu.VMEM((2, PAIR, d_model), bf16),
            pltpu.VMEM((SLOT_ROWS, d_model), f32),
            pltpu.VMEM((LOCAL_ROWS, d_model), bf16),
            pltpu.VMEM((N_SEG * SEG, d_model), bf16),
            pltpu.VMEM((2, PAIR, d_model), bf16),
            pltpu.VMEM((EARLY_ROWS, d_model), bf16),
            pltpu.VMEM((n_tok, d_model), bf16),
            pltpu.VMEM((n_tok, LAST_ROWS), bf16),
            pltpu.VMEM((3 * SEG, 128), f32),
            pltpu.VMEM((8, n_tok), jnp.int32),
            pltpu.VMEM((8, n_tok), jnp.int32),
            pltpu.VMEM((n_tok, 128), jnp.int32),
            pltpu.VMEM((n_tok, 128), f32),
            pltpu.VMEM((2, 8, 128), f32),
            pltpu.VMEM((2, 8, 128), f32),
            pltpu.VMEM((6, 8, 128), f32),
            dma((6,)), dma((n_slot, 2)),
            dma((N_SEG, 3)), dma((N_SEG, 3)), dma((N_SEG, 3)), dma((N_SEG, 3)),
            dma((n_tok // 256,)), dma((2,)), dma((2,)), dma((4,)), dma((4,)),
        ],
        compiler_params=pltpu.CompilerParams(collective_id=0, has_side_effects=True, vmem_limit_bytes=60 * 1024 * 1024),
    )(slot_expert, topk_idx.reshape(1, n_tok), topk_w.reshape(1, n_tok), tokens, w_up[0], w_down[0])


def solution(mesh):
    def group_layer(tokens, topk_idx, topk_w, w_up, w_down, slot_expert):
        *parts, found = fast_layer(tokens, topk_idx, topk_w, w_up, w_down, slot_expert)
        args = (*parts, tokens, topk_idx, topk_w, w_up, w_down, slot_expert)
        return lax.cond(found[0, 0] == 1, lambda *a: add_last(*a[:4]), lambda *a: general_layer(*a[4:]), *args)

    row_spec = P(('dp', 'ep'), None)
    weight_spec = P('ep', None, None, None)
    return jax.shard_map(group_layer, mesh=mesh, in_specs=(row_spec, row_spec, row_spec, weight_spec, weight_spec, P(None, None)), out_specs=row_spec, check_vma=False)
```

```python
import functools

import jax
import jax.numpy as jnp
from jax import lax
from jax.experimental import pallas as pl
from jax.experimental.pallas import tpu as pltpu
from jax.sharding import PartitionSpec as P

MAX_COPIES = 4
SEG = 80
N_SEG = 4
DIRECT = 240
SHARED = 64
SEND_AT = (0, 80, 160, 240)
BACK_AT = (0, 48, 112, 192, 240)
SLOT_ROWS = 4 * SEG
STREAM_AT = (None, 0, N_SEG * SEG, N_SEG * SEG + DIRECT)
SHARED_AT = N_SEG * SEG + 2 * DIRECT
RAW_AT = (None, None, 4096, 6144)
LOCAL_BASE = 1024
LOCAL_ROWS = 1664
LAST_ROWS = 256
EARLY_ROWS = 640
FF_TILE = 1536
N_WBUF = 4
MESH = pl.DeviceIdType.MESH


def slot_bound(n_tok, n_top, n_dev, n_slot):
    base_load = (n_tok * n_top) // (n_dev * n_slot)
    return base_load + base_load // 2 + 1


def route_pairs(topk_idx, slot_expert, capacity):
    n_dev, n_slot = slot_expert.shape
    n_exp = n_dev * (n_slot - 1)
    n_top = topk_idx.shape[1]
    table_flat = slot_expert.reshape(-1)
    slot_ids = jnp.arange(n_dev * n_slot, dtype=jnp.int32)
    same_exp = table_flat[:, None] == table_flat[None, :]
    earlier = slot_ids[None, :] < slot_ids[:, None]
    copy_rank = jnp.sum(same_exp & earlier, axis=1, dtype=jnp.int32)
    exp_copies = jax.ops.segment_sum(jnp.ones_like(table_flat), table_flat, num_segments=n_exp)
    slot_of = jnp.zeros((n_exp, MAX_COPIES), jnp.int32).at[table_flat, copy_rank].set(slot_ids)
    flat_exp = topk_idx.reshape(-1)
    onehot = (flat_exp[:, None] == jnp.arange(n_exp, dtype=jnp.int32)[None, :]).astype(jnp.int32)
    pair_rank = jnp.sum((jnp.cumsum(onehot, axis=0) - onehot) * onehot, axis=1)
    pair_copies = exp_copies[flat_exp]
    slot_flat = slot_of[flat_exp, pair_rank % pair_copies]
    buf_row = pair_rank // pair_copies
    pair_pos = ((slot_flat % n_slot) * n_dev + slot_flat // n_slot) * capacity + buf_row
    pair_tok = jnp.arange(flat_exp.shape[0], dtype=jnp.int32) // n_top
    buf_tok = jnp.zeros((n_slot * n_dev * capacity,), jnp.int32).at[pair_pos].set(pair_tok)
    return pair_pos, buf_tok


def expert_ffn(recv_buf, up_local, down_local):
    pre_act = jnp.einsum('spcm,smf->spcf', recv_buf, up_local, preferred_element_type=jnp.float32)
    hidden = jax.nn.gelu(pre_act, approximate=True).astype(jnp.bfloat16)
    return jnp.einsum('spcf,sfm->spcm', hidden, down_local, preferred_element_type=jnp.float32).astype(jnp.bfloat16)


def general_layer(tokens, topk_idx, topk_w, w_up, w_down, slot_expert):
    n_tok, d_model = tokens.shape
    n_top = topk_idx.shape[1]
    n_dev, n_slot = slot_expert.shape
    capacity = slot_bound(n_tok, n_top, n_dev, n_slot)
    pair_pos, buf_tok = route_pairs(topk_idx, slot_expert, capacity)
    send_buf = tokens[buf_tok].reshape(n_slot, n_dev, capacity, d_model)
    recv_buf = lax.all_to_all(send_buf, 'ep', 1, 1, tiled=True)
    expert_out = expert_ffn(recv_buf, w_up[0], w_down[0])
    back_buf = lax.all_to_all(expert_out, 'ep', 1, 1, tiled=True)
    pair_out = back_buf.reshape(-1, d_model)[pair_pos]
    return (pair_out.astype(jnp.float32) * topk_w).astype(jnp.bfloat16)


def stream_starts(counts, hot_slot):
    out_at, back_at = [], []
    out_end = back_end = jnp.zeros_like(counts[0])
    for s, count in enumerate(counts):
        out_at.append(out_end)
        floor = jnp.where(hot_slot < s, float(BACK_AT[max(s - 1, 0)]), float(BACK_AT[min(s, N_SEG - 1)]))
        start = jnp.where(hot_slot == s, back_end, jnp.maximum(back_end, floor))
        back_at.append(start)
        out_end = out_end + count
        back_end = start + count
    return out_at, back_at, out_end, back_end


def route(idx_row, table, peers, n_exp, n_slot):
    f32 = jnp.float32
    n_tok = idx_row.shape[1]
    lanes = 128
    onehot = (lax.broadcasted_iota(jnp.int32, (n_exp, n_tok), 0) == idx_row).astype(f32)
    step = 256
    blocks = [onehot[:, b * step:(b + 1) * step] for b in range(n_tok // step)]
    before = lax.broadcasted_iota(jnp.int32, (step, step), 0) < lax.broadcasted_iota(jnp.int32, (step, step), 1)
    local_rank = jnp.dot(jnp.concatenate(blocks, axis=0).astype(jnp.bfloat16), before.astype(f32).astype(jnp.bfloat16), preferred_element_type=f32)
    carry = jnp.zeros((n_exp, 1), f32)
    ranks = []
    for b, block in enumerate(blocks):
        ranks.append(local_rank[b * n_exp:(b + 1) * n_exp] + carry)
        carry = carry + jnp.sum(block, axis=1, keepdims=True)
    rank = jnp.concatenate(ranks, axis=1)
    n_pair = jnp.broadcast_to(carry, (n_exp, lanes))

    exp_id = lax.broadcasted_iota(jnp.int32, (n_exp, lanes), 0)
    match = [[(exp_id == table[d, s]).astype(f32) for s in range(n_slot)] for d in peers]
    copies = sum(sum(row) for row in match)
    per_copy = 1.0 / copies
    hot = (copies == 4.0).astype(f32)
    own = sum(match[0])
    own_slot = sum(s * match[0][s] for s in range(n_slot))
    seen = jnp.zeros((n_exp, lanes), f32)
    start_out = [jnp.zeros((n_exp, lanes), f32) for _ in range(MAX_COPIES)]
    start_back = [jnp.zeros((n_exp, lanes), f32) for _ in range(MAX_COPIES)]
    stream_counts, over_out, over_back = [], [], []
    for r in range(len(peers)):
        seens, counts = [], []
        peer_hot = jnp.zeros((1, lanes), f32)
        for s in range(n_slot):
            here = match[r][s]
            seens.append(seen)
            rows = jnp.floor((n_pair - seen + copies - 0.5) * per_copy)
            counts.append(jnp.sum(here * (1.0 - own) * rows, axis=0, keepdims=True))
            peer_hot = peer_hot + s * jnp.sum(here * hot, axis=0, keepdims=True)
            seen = seen + here
        out_at, back_at, out_end, back_end = stream_starts(counts, peer_hot)
        if r == 0:
            hot_slot = peer_hot
        if r >= 2:
            stream_counts.append(counts)
            over_out.append(jnp.maximum(out_end - DIRECT, 0.0))
            over_back.append(jnp.maximum(back_end - DIRECT, 0.0))
        for s in range(n_slot):
            local = LOCAL_BASE + SLOT_ROWS * own_slot + SEG * r
            if r == 0:
                code_out = code_back = local
            elif r == 1:
                seg = s - (peer_hot < s).astype(f32)
                code_out = code_back = jnp.where(own > 0, local, STREAM_AT[1] + SEG * seg)
            else:
                code_out = jnp.where(own > 0, local, RAW_AT[r] + out_at[s])
                code_back = jnp.where(own > 0, local, RAW_AT[r] + back_at[s])
            for c in range(MAX_COPIES):
                mine = (match[r][s] > 0) & (seens[s] == c)
                start_out[c] = jnp.where(mine, code_out, start_out[c])
                start_back[c] = jnp.where(mine, code_back, start_back[c])

    wide = lambda a: jnp.concatenate([a] * (n_tok // lanes), axis=1)
    row = jnp.floor((rank + 0.5) * wide(per_copy))
    which = rank - row * wide(copies)
    codes = []
    for starts, over in ((start_out, over_out), (start_back, over_back)):
        start = wide(starts[3])
        for c in range(MAX_COPIES - 1):
            start = jnp.where(which == c, wide(starts[c]), start)
        raw = jnp.sum(onehot * (start + row), axis=0, keepdims=True)
        code = raw
        for r, first in ((2, 0.0), (3, over[0][:, :1])):
            at = raw - RAW_AT[r]
            code = jnp.where(at >= 0, jnp.where(at < DIRECT, STREAM_AT[r] + at, SHARED_AT + first + (at - DIRECT)), code)
        codes.append(code.astype(jnp.int32))
    over = jnp.maximum(over_out[0] + over_out[1], over_back[0] + over_back[1])
    fits = jnp.max(own * hot, axis=0, keepdims=True) * (over <= SHARED).astype(f32)
    zero = jnp.zeros((1, lanes), f32)
    tables = [jnp.concatenate(stream_counts[0] + [zero] * (8 - n_slot), axis=0),
              jnp.concatenate(stream_counts[1] + [over_out[0], over_back[0]] + [zero] * (6 - n_slot), axis=0)]
    return codes, hot_slot, tables, fits


def layer_kernel(slot_expert, topk_idx, topk_w, tokens, w_up, w_down, out, last_rows, last_mask, last_gate, found, table, idx_row, gate_row, tok_buf, up_buf, down_buf, send_core, recv_core, send_chip, send_shared, recv_chip, acc, rows_buf, back_core, back_chip, back_shared, swap_out, swap_in, early, mixed, mask_buf, gate_buf, code_row, back_row, code_col, gate_col, counts_out, counts_in, flags, t_sem, w_sem, ds_sem, dr_sem, bs_sem, br_sem, o_sem, cs_sem, cr_sem, fs_sem, fr_sem, xs_sem, xr_sem):
    f32, bf16 = jnp.float32, jnp.bfloat16
    n_tok, d_model = tok_buf.shape
    n_slot = w_up.shape[0]
    d_ff = w_up.shape[2]
    me = lax.axis_index('ep')
    group = lax.axis_index('dp')
    chip, core = me // 2, me % 2
    peers = [me, 2 * chip + (1 - core), 2 * (1 - chip) + core, 2 * (1 - chip) + (1 - core)]
    peer_ids = [None] + [{'ep': peers[r]} for r in (1, 2, 3)] + [{'dp': 1 - group}]

    barrier = pltpu.get_barrier_semaphore()
    for r in (1, 2, 3, 4):
        pl.semaphore_signal(barrier, inc=1, device_id=peer_ids[r], device_id_type=MESH)

    def weight_copies(s):
        b = s % N_WBUF
        return (pltpu.make_async_copy(w_up.at[s], up_buf.at[b], w_sem.at[s, 0]),
                pltpu.make_async_copy(w_down.at[s], down_buf.at[b], w_sem.at[s, 1]))

    small_copies = [pltpu.make_async_copy(slot_expert, table, t_sem.at[0]),
                    pltpu.make_async_copy(topk_idx, idx_row, t_sem.at[1]),
                    pltpu.make_async_copy(topk_w, gate_row, t_sem.at[2])]
    token_copy = pltpu.make_async_copy(tokens, tok_buf, t_sem.at[3])
    for copy in small_copies:
        copy.start()
    token_copy.start()
    for copy in small_copies:
        copy.wait()
    (code_out, code_back), hot_slot, count_tables, fits = route(idx_row[...], table, peers, 16, n_slot)
    code_row[...] = jnp.broadcast_to(code_out, code_row.shape)
    back_row[...] = jnp.broadcast_to(code_back, back_row.shape)
    hot_slot = hot_slot[:, :1]
    for r in (2, 3):
        counts_out[r - 2] = count_tables[r - 2]
    flags[0] = jnp.broadcast_to(fits, (8, 128))

    def pick(ids):
        mask = (ids == code_row[0:1, :]).astype(f32).astype(bf16)
        return jnp.dot(mask, tok_buf[...], preferred_element_type=f32).astype(bf16)

    def ids_from(first, rows):
        return lax.broadcasted_iota(jnp.int32, (rows, n_tok), 0) + first

    def dispatch_copy(k, r):
        to = r
        if r == 1:
            rows = pl.ds(k * SEG, SEG)
            src, dst = send_core.at[rows], recv_core.at[rows]
        elif k < N_SEG - 1:
            rows = pl.ds(SEND_AT[k], SEND_AT[k + 1] - SEND_AT[k])
            src, dst = send_chip.at[r - 2, rows], recv_chip.at[r - 2, rows]
        elif r == 2:
            src, dst = send_shared, recv_chip.at[0, pl.ds(DIRECT, SHARED)]
        else:
            to = 1
            src, dst = recv_chip.at[0, pl.ds(DIRECT, SHARED)], recv_chip.at[1, pl.ds(DIRECT, SHARED)]
        return pltpu.make_async_remote_copy(
            src_ref=src, dst_ref=dst, send_sem=ds_sem.at[k, r - 1], recv_sem=dr_sem.at[k, r - 1],
            device_id=peer_ids[to], device_id_type=MESH)

    def back_copy(k, r):
        size = BACK_AT[k + 1] - BACK_AT[k]
        if r == 1:
            src, to_early, to_last = back_core.at[pl.ds(k * SEG, SEG)], pl.ds(k * SEG, SEG), pl.ds(0, SEG)
        else:
            src = back_chip.at[r - 2, pl.ds(BACK_AT[k], size)]
            to_early = pl.ds(3 * SEG + (r - 2) * BACK_AT[3] + BACK_AT[k], size)
            to_last = pl.ds(SEG + (r - 2) * size, size)
        return pltpu.make_async_remote_copy(
            src_ref=src, dst_ref=early.at[to_early] if k < N_SEG - 1 else last_rows.at[to_last],
            send_sem=bs_sem.at[k, r - 1], recv_sem=br_sem.at[k, r - 1],
            device_id=peer_ids[r], device_id_type=MESH)

    last_size = BACK_AT[N_SEG] - BACK_AT[N_SEG - 1]

    def shared_copy(r):
        if r == 1:
            src, dst = swap_out, swap_in
        else:
            src, dst = back_shared, last_rows.at[pl.ds(SEG + 2 * last_size, SHARED)]
        return pltpu.make_async_remote_copy(
            src_ref=src, dst_ref=dst, send_sem=xs_sem.at[r - 1], recv_sem=xr_sem.at[r - 1],
            device_id=peer_ids[r], device_id_type=MESH)

    def counts_copy(r):
        return pltpu.make_async_remote_copy(
            src_ref=counts_out.at[r - 2], dst_ref=counts_in.at[r - 2], send_sem=cs_sem.at[r - 2], recv_sem=cr_sem.at[r - 2],
            device_id=peer_ids[r], device_id_type=MESH)

    def flag_copy(r):
        src, dst = (0, 1) if r == 4 else (2, 2 + r)
        return pltpu.make_async_remote_copy(
            src_ref=flags.at[src], dst_ref=flags.at[dst], send_sem=fs_sem.at[r - 1], recv_sem=fr_sem.at[r - 1],
            device_id=peer_ids[r], device_id_type=MESH)

    token_copy.wait()
    for s in range(N_WBUF):
        for copy in weight_copies(s):
            copy.start()
    for k in range(N_SEG):
        if k < N_SEG - 1:
            size = SEND_AT[k + 1] - SEND_AT[k]
            ids = [ids_from(STREAM_AT[2] + SEND_AT[k], size), ids_from(STREAM_AT[3] + SEND_AT[k], size), ids_from(k * SEG, SEG)]
            picked = pick(jnp.concatenate(ids, axis=0))
            send_chip[0, SEND_AT[k]:SEND_AT[k + 1], :] = picked[:size]
            send_chip[1, SEND_AT[k]:SEND_AT[k + 1], :] = picked[size:2 * size]
        else:
            picked = pick(jnp.concatenate([ids_from(SHARED_AT, SHARED), ids_from(k * SEG, SEG)], axis=0))
            send_shared[...] = picked[:SHARED]
        send_core[k * SEG:(k + 1) * SEG, :] = picked[-SEG:]
        if k == 0:
            pl.semaphore_wait(barrier, 4)
            for r in (2, 3):
                counts_copy(r).start()
        for r in (2, 3, 1) if k < N_SEG - 1 else (2, 1):
            dispatch_copy(k, r).start()
    flag_copy(4).start()

    for s in range(n_slot):
        rows_buf[s * SLOT_ROWS:(s + 1) * SLOT_ROWS, :] = pick(ids_from(LOCAL_BASE + s * SLOT_ROWS, SLOT_ROWS))
    code_col[...] = jnp.transpose(jnp.broadcast_to(code_back, (128, n_tok)))
    gate_col[...] = jnp.transpose(jnp.broadcast_to(gate_row[...], (128, n_tok)))
    n_early = 3 * SEG + 2 * BACK_AT[3]
    early[n_early:, :] = jnp.zeros((EARLY_ROWS - n_early, d_model), bf16)
    rows_buf[n_slot * SLOT_ROWS:, :] = jnp.zeros((LOCAL_ROWS - n_slot * SLOT_ROWS, d_model), bf16)

    def piecewise(i, pieces):
        ids, at = jnp.full_like(i, -1), sum(size for _, size in pieces)
        for first, size in reversed(pieces):
            ids = jnp.where(i < at, i + (first - at + size), ids)
            at -= size
        return ids

    last_ids = lambda i: piecewise(i, [(STREAM_AT[1] + 3 * SEG, SEG), (STREAM_AT[2] + BACK_AT[3], last_size),
                                       (STREAM_AT[3] + BACK_AT[3], last_size), (SHARED_AT, SHARED)])
    early_ids = lambda i: piecewise(i, [(STREAM_AT[1], 3 * SEG), (STREAM_AT[2], BACK_AT[3]), (STREAM_AT[3], BACK_AT[3])])
    n_last = SEG + 2 * last_size + SHARED

    ids = last_ids(lax.broadcasted_iota(jnp.int32, (n_last, n_tok), 0))
    gates = jnp.sum(jnp.where(ids == back_row[0:1, :], gate_row[...], 0.0), axis=1, keepdims=True)
    gate_buf[...] = jnp.broadcast_to(gates, gate_buf.shape)
    lane = lax.broadcasted_iota(jnp.int32, (n_tok, 128), 1)
    for j in range(LAST_ROWS // 128):
        mask_buf[:, j * 128:(j + 1) * 128] = (code_col[...] == last_ids(lane + 128 * j)).astype(f32).astype(bf16)
    side_copies = [pltpu.make_async_copy(mask_buf, last_mask, t_sem.at[4]),
                   pltpu.make_async_copy(gate_buf, last_gate, t_sem.at[5])]
    for copy in side_copies:
        copy.start()
    flag_copy(4).wait_recv()
    flags[2] = jnp.minimum(flags[0], flags[1])
    for r in (1, 2, 3):
        flag_copy(r).start()
    for r in (2, 3):
        counts_copy(r).wait_recv()
    in_counts = [[counts_in[j, s:s + 1, :1] for s in range(n_slot)] for j in range(2)]
    in_first = [[counts_in[j, n_slot + d:n_slot + d + 1, :1] for d in range(2)] for j in range(2)]
    in_starts = [stream_starts(counts, hot_slot) for counts in in_counts]
    as_int = lambda a: a.astype(jnp.int32)

    def returned(r, first, size, slots, shift):
        slots = list(slots)
        i = lax.broadcasted_iota(jnp.int32, (size, SEG * len(slots)), 0)
        j = lax.broadcasted_iota(jnp.int32, (size, SEG * len(slots)), 1)
        mask = jnp.zeros(i.shape, f32)
        for n, q in enumerate(slots):
            row = j - n * SEG
            at = row + as_int(in_starts[r - 2][1][q])
            fit = (at + shift == i + first) & (at >= first) & (row >= 0) & (row < as_int(in_counts[r - 2][q]))
            mask = jnp.where(fit, 1.0, mask)
        done = jnp.concatenate([rows_buf[q * SLOT_ROWS + r * SEG:q * SLOT_ROWS + (r + 1) * SEG, :] for q in slots], axis=0)
        return jnp.dot(mask.astype(bf16), done, preferred_element_type=f32).astype(bf16)

    for s in range(n_slot):
        lo, hi = s * SLOT_ROWS, (s + 1) * SLOT_ROWS
        if s < N_SEG:
            for r in (1, 2, 3) if s < N_SEG - 1 else (1, 3):
                dispatch_copy(s, r).wait_recv()
        near = rows_buf[lo + SEG:lo + 2 * SEG, :].astype(f32)
        if s < N_SEG:
            near = near + recv_core[s * SEG:(s + 1) * SEG, :].astype(f32) * (hot_slot > s).astype(f32)
        if s > 0:
            near = near + recv_core[(s - 1) * SEG:s * SEG, :].astype(f32) * (hot_slot < s).astype(f32)
        rows_buf[lo + SEG:lo + 2 * SEG, :] = near.astype(bf16)
        come = SEND_AT[s + 1] if s < N_SEG - 1 else DIRECT + SHARED
        i = lax.broadcasted_iota(jnp.int32, (SEG, come), 0)
        j = lax.broadcasted_iota(jnp.int32, (SEG, come), 1)
        for r in (2, 3):
            at = i + as_int(in_starts[r - 2][0][s])
            if s >= N_SEG - 1:
                at = jnp.where(at < DIRECT, at, at + as_int(in_first[r - 2][0]))
            mask = (j == at) & (i < as_int(in_counts[r - 2][s]))
            far = jnp.dot(mask.astype(f32).astype(bf16), recv_chip[r - 2, :come, :], preferred_element_type=f32)
            at = slice(lo + r * SEG, lo + (r + 1) * SEG)
            rows_buf[at, :] = (rows_buf[at, :].astype(f32) + far).astype(bf16)
        for copy in weight_copies(s):
            copy.wait()
        b = s % N_WBUF
        acc[...] = jnp.zeros_like(acc)

        def ff_step(i, carry):
            cols = pl.ds(pl.multiple_of(i * FF_TILE, FF_TILE), FF_TILE)
            pre = jnp.dot(rows_buf[lo:hi, :], up_buf[b, :, cols], preferred_element_type=f32)
            hidden = jax.nn.gelu(pre, approximate=True).astype(bf16)
            acc[...] += jnp.dot(hidden, down_buf[b, cols, :], preferred_element_type=f32)
            return carry

        lax.fori_loop(0, d_ff // FF_TILE, ff_step, 0)
        if s + N_WBUF < n_slot:
            for copy in weight_copies(s + N_WBUF):
                copy.start()
        rows_buf[lo:hi, :] = acc[...].astype(bf16)
        if s == N_SEG - 2:
            dispatch_copy(N_SEG - 1, 2).wait_recv()
            dispatch_copy(N_SEG - 1, 3).start()
        if s > 0:
            k = s - 1
            if k == N_SEG - 1:
                swap_out[...] = returned(3, DIRECT, SHARED, (s - 1, s), as_int(in_first[1][1]))
                shared_copy(1).start()
            for r in (2, 3):
                back_chip[r - 2, BACK_AT[k]:BACK_AT[k + 1], :] = returned(r, BACK_AT[k], BACK_AT[k + 1] - BACK_AT[k], range(max(k - 2, 0), s + 1), 0)
                back_copy(k, r).start()
            prev = rows_buf[lo - SLOT_ROWS + SEG:lo - SLOT_ROWS + 2 * SEG, :].astype(f32)
            last = rows_buf[lo + SEG:lo + 2 * SEG, :].astype(f32)
            back = prev * (hot_slot > k).astype(f32) + last * (hot_slot <= k).astype(f32)
            back_core[k * SEG:(k + 1) * SEG, :] = back.astype(bf16)
            back_copy(k, 1).start()
            if k == N_SEG - 1:
                mine = returned(2, DIRECT, SHARED, (s - 1, s), as_int(in_first[0][1]))
                shared_copy(1).wait_recv()
                back_shared[...] = (mine.astype(f32) + swap_in[...].astype(f32)).astype(bf16)
                shared_copy(2).start()

    tile = 256
    n_tile = n_tok // tile

    def out_copy(i):
        at = pl.ds(pl.multiple_of(i * tile, tile), tile)
        return pltpu.make_async_copy(mixed.at[at], out.at[at], o_sem.at[i])

    def combine(ids_of, rows, source, final):
        def body(i, carry):
            at = pl.ds(pl.multiple_of(i * tile, tile), tile)
            mine = code_col[at, :]
            lane = lax.broadcasted_iota(jnp.int32, (tile, 128), 1)
            mask = jnp.concatenate([(mine == ids_of(lane + 128 * j)).astype(f32).astype(bf16) for j in range(rows // 128)], axis=1)
            part = jnp.dot(mask, source[...], preferred_element_type=f32)
            if final:
                part = part + mixed[at, :].astype(f32)
                part = part * jnp.concatenate([gate_col[at, :]] * (d_model // 128), axis=1)
            mixed[at, :] = part.astype(bf16)
            if final:
                out_copy(i).start()
            return carry
        lax.fori_loop(0, n_tile, body, 0)

    combine(lambda i: LOCAL_BASE + i, LOCAL_ROWS, rows_buf, False)
    for r in (1, 2, 3):
        flag_copy(r).wait_recv()
    agreed = jnp.minimum(jnp.minimum(flags[2], flags[3]), jnp.minimum(flags[4], flags[5]))
    found[...] = agreed[0:1, :].astype(jnp.int32)
    for k in range(N_SEG):
        for r in (1, 2, 3):
            back_copy(k, r).wait_recv()
        if k == N_SEG - 1:
            shared_copy(2).wait_recv()
        if k == N_SEG - 2:
            combine(early_ids, EARLY_ROWS, early, True)
            for i in range(n_tile):
                out_copy(i).wait()
            for copy in side_copies:
                copy.wait()
    for r in (2, 3):
        counts_copy(r).wait_send()
    for r in (1, 2):
        shared_copy(r).wait_send()
    for r in (1, 2, 3, 4):
        flag_copy(r).wait_send()
    for k in range(N_SEG):
        for r in (1, 2, 3):
            dispatch_copy(k, r).wait_send()
            back_copy(k, r).wait_send()


def last_kernel(part, rows, mask, gate, out):
    f32, bf16 = jnp.float32, jnp.bfloat16
    d_model = part.shape[1]
    gates = jnp.concatenate([gate[...]] * (d_model // 128), axis=1)
    scaled = (rows[...].astype(f32) * gates).astype(bf16)
    scaled = jnp.concatenate([scaled, jnp.zeros((LAST_ROWS - scaled.shape[0], d_model), bf16)], axis=0)
    late = jnp.dot(mask[...], scaled, preferred_element_type=f32)
    out[...] = (late + part[...].astype(f32)).astype(bf16)


def add_last(part, rows, mask, gate):
    n_tok, d_model = part.shape
    tile = 512
    by_tile = lambda cols: pl.BlockSpec((tile, cols), lambda i: (i, 0))
    whole = lambda a: pl.BlockSpec(a.shape, lambda i: (0, 0))
    return pl.pallas_call(
        last_kernel,
        grid=(n_tok // tile,),
        out_shape=jax.ShapeDtypeStruct(part.shape, part.dtype),
        in_specs=[by_tile(d_model), whole(rows), by_tile(mask.shape[1]), whole(gate)],
        out_specs=by_tile(d_model),
    )(part, rows, mask, gate)


def fast_layer(tokens, topk_idx, topk_w, w_up, w_down, slot_expert):
    n_tok, d_model = tokens.shape
    n_slot, d_ff = w_up.shape[1], w_up.shape[3]
    vmem = pl.BlockSpec(memory_space=pltpu.VMEM)
    anym = pl.BlockSpec(memory_space=pl.ANY)
    bf16, f32 = jnp.bfloat16, jnp.float32
    shape = jax.ShapeDtypeStruct
    dma = pltpu.SemaphoreType.DMA
    return pl.pallas_call(
        layer_kernel,
        out_shape=(shape((n_tok, d_model), bf16), shape((3 * SEG, d_model), bf16), shape((n_tok, LAST_ROWS), bf16),
                   shape((3 * SEG, 128), f32), shape((1, 128), jnp.int32)),
        in_specs=[anym] * 6,
        out_specs=(anym, anym, anym, anym, vmem),
        scratch_shapes=[
            pltpu.SMEM(slot_expert.shape, jnp.int32),
            pltpu.VMEM((1, n_tok), jnp.int32),
            pltpu.VMEM((1, n_tok), f32),
            pltpu.VMEM((n_tok, d_model), bf16),
            pltpu.VMEM((N_WBUF, d_model, d_ff), bf16),
            pltpu.VMEM((N_WBUF, d_ff, d_model), bf16),
            pltpu.VMEM((N_SEG * SEG, d_model), bf16),
            pltpu.VMEM((N_SEG * SEG, d_model), bf16),
            pltpu.VMEM((2, DIRECT, d_model), bf16),
            pltpu.VMEM((SHARED, d_model), bf16),
            pltpu.VMEM((2, DIRECT + SHARED, d_model), bf16),
            pltpu.VMEM((SLOT_ROWS, d_model), f32),
            pltpu.VMEM((LOCAL_ROWS, d_model), bf16),
            pltpu.VMEM((N_SEG * SEG, d_model), bf16),
            pltpu.VMEM((2, DIRECT, d_model), bf16),
            pltpu.VMEM((SHARED, d_model), bf16),
            pltpu.VMEM((SHARED, d_model), bf16),
            pltpu.VMEM((SHARED, d_model), bf16),
            pltpu.VMEM((EARLY_ROWS, d_model), bf16),
            pltpu.VMEM((n_tok, d_model), bf16),
            pltpu.VMEM((n_tok, LAST_ROWS), bf16),
            pltpu.VMEM((3 * SEG, 128), f32),
            pltpu.VMEM((8, n_tok), jnp.int32),
            pltpu.VMEM((8, n_tok), jnp.int32),
            pltpu.VMEM((n_tok, 128), jnp.int32),
            pltpu.VMEM((n_tok, 128), f32),
            pltpu.VMEM((2, 8, 128), f32),
            pltpu.VMEM((2, 8, 128), f32),
            pltpu.VMEM((6, 8, 128), f32),
            dma((6,)), dma((n_slot, 2)),
            dma((N_SEG, 3)), dma((N_SEG, 3)), dma((N_SEG, 3)), dma((N_SEG, 3)),
            dma((n_tok // 256,)), dma((2,)), dma((2,)), dma((4,)), dma((4,)), dma((2,)), dma((2,)),
        ],
        compiler_params=pltpu.CompilerParams(collective_id=0, has_side_effects=True, vmem_limit_bytes=60 * 1024 * 1024),
    )(slot_expert, topk_idx.reshape(1, n_tok), topk_w.reshape(1, n_tok), tokens, w_up[0], w_down[0])


def solution(mesh):
    def group_layer(tokens, topk_idx, topk_w, w_up, w_down, slot_expert):
        *parts, found = fast_layer(tokens, topk_idx, topk_w, w_up, w_down, slot_expert)
        args = (*parts, tokens, topk_idx, topk_w, w_up, w_down, slot_expert)
        return lax.cond(found[0, 0] == 1, lambda *a: add_last(*a[:4]), lambda *a: general_layer(*a[4:]), *args)

    row_spec = P(('dp', 'ep'), None)
    weight_spec = P('ep', None, None, None)
    return jax.shard_map(group_layer, mesh=mesh, in_specs=(row_spec, row_spec, row_spec, weight_spec, weight_spec, P(None, None)), out_specs=row_spec, check_vma=False)
```

```python
import functools

import jax
import jax.numpy as jnp
from jax import lax
from jax.experimental import pallas as pl
from jax.experimental.pallas import tpu as pltpu
from jax.sharding import PartitionSpec as P

MAX_COPIES = 4
SEG = 80
N_SEG = 4
DIRECT = 240
SHARED = 64
SEND_AT = (0, 80, 160, 240)
BACK_AT = (0, 48, 112, 192, 240)
SLOT_ROWS = 4 * SEG
STREAM_AT = (None, 0, N_SEG * SEG, N_SEG * SEG + DIRECT)
SHARED_AT = N_SEG * SEG + 2 * DIRECT
RAW_AT = (None, None, 4096, 6144)
LOCAL_BASE = 1024
LOCAL_ROWS = 1664
LAST_ROWS = 256
EARLY_ROWS = 640
FF_TILE = 1536
N_WBUF = 4
MESH = pl.DeviceIdType.MESH


def slot_bound(n_tok, n_top, n_dev, n_slot):
    base_load = (n_tok * n_top) // (n_dev * n_slot)
    return base_load + base_load // 2 + 1


def route_pairs(topk_idx, slot_expert, capacity):
    n_dev, n_slot = slot_expert.shape
    n_exp = n_dev * (n_slot - 1)
    n_top = topk_idx.shape[1]
    table_flat = slot_expert.reshape(-1)
    slot_ids = jnp.arange(n_dev * n_slot, dtype=jnp.int32)
    same_exp = table_flat[:, None] == table_flat[None, :]
    earlier = slot_ids[None, :] < slot_ids[:, None]
    copy_rank = jnp.sum(same_exp & earlier, axis=1, dtype=jnp.int32)
    exp_copies = jax.ops.segment_sum(jnp.ones_like(table_flat), table_flat, num_segments=n_exp)
    slot_of = jnp.zeros((n_exp, MAX_COPIES), jnp.int32).at[table_flat, copy_rank].set(slot_ids)
    flat_exp = topk_idx.reshape(-1)
    onehot = (flat_exp[:, None] == jnp.arange(n_exp, dtype=jnp.int32)[None, :]).astype(jnp.int32)
    pair_rank = jnp.sum((jnp.cumsum(onehot, axis=0) - onehot) * onehot, axis=1)
    pair_copies = exp_copies[flat_exp]
    slot_flat = slot_of[flat_exp, pair_rank % pair_copies]
    buf_row = pair_rank // pair_copies
    pair_pos = ((slot_flat % n_slot) * n_dev + slot_flat // n_slot) * capacity + buf_row
    pair_tok = jnp.arange(flat_exp.shape[0], dtype=jnp.int32) // n_top
    buf_tok = jnp.zeros((n_slot * n_dev * capacity,), jnp.int32).at[pair_pos].set(pair_tok)
    return pair_pos, buf_tok


def expert_ffn(recv_buf, up_local, down_local):
    pre_act = jnp.einsum('spcm,smf->spcf', recv_buf, up_local, preferred_element_type=jnp.float32)
    hidden = jax.nn.gelu(pre_act, approximate=True).astype(jnp.bfloat16)
    return jnp.einsum('spcf,sfm->spcm', hidden, down_local, preferred_element_type=jnp.float32).astype(jnp.bfloat16)


def general_layer(tokens, topk_idx, topk_w, w_up, w_down, slot_expert):
    n_tok, d_model = tokens.shape
    n_top = topk_idx.shape[1]
    n_dev, n_slot = slot_expert.shape
    capacity = slot_bound(n_tok, n_top, n_dev, n_slot)
    pair_pos, buf_tok = route_pairs(topk_idx, slot_expert, capacity)
    send_buf = tokens[buf_tok].reshape(n_slot, n_dev, capacity, d_model)
    recv_buf = lax.all_to_all(send_buf, 'ep', 1, 1, tiled=True)
    expert_out = expert_ffn(recv_buf, w_up[0], w_down[0])
    back_buf = lax.all_to_all(expert_out, 'ep', 1, 1, tiled=True)
    pair_out = back_buf.reshape(-1, d_model)[pair_pos]
    return (pair_out.astype(jnp.float32) * topk_w).astype(jnp.bfloat16)


def stream_starts(counts, hot_slot):
    out_at, back_at = [], []
    out_end = back_end = jnp.zeros_like(counts[0])
    for s, count in enumerate(counts):
        out_at.append(out_end)
        floor = jnp.where(hot_slot < s, float(BACK_AT[max(s - 1, 0)]), float(BACK_AT[min(s, N_SEG - 1)]))
        start = jnp.where(hot_slot == s, back_end, jnp.maximum(back_end, floor))
        back_at.append(start)
        out_end = out_end + count
        back_end = start + count
    return out_at, back_at, out_end, back_end


def route(idx_row, table, peers, n_exp, n_slot):
    f32 = jnp.float32
    n_tok = idx_row.shape[1]
    lanes = 128
    onehot = (lax.broadcasted_iota(jnp.int32, (n_exp, n_tok), 0) == idx_row).astype(f32)
    step = 256
    blocks = [onehot[:, b * step:(b + 1) * step] for b in range(n_tok // step)]
    before = lax.broadcasted_iota(jnp.int32, (step, step), 0) < lax.broadcasted_iota(jnp.int32, (step, step), 1)
    local_rank = jnp.dot(jnp.concatenate(blocks, axis=0).astype(jnp.bfloat16), before.astype(f32).astype(jnp.bfloat16), preferred_element_type=f32)
    carry = jnp.zeros((n_exp, 1), f32)
    ranks = []
    for b, block in enumerate(blocks):
        ranks.append(local_rank[b * n_exp:(b + 1) * n_exp] + carry)
        carry = carry + jnp.sum(block, axis=1, keepdims=True)
    rank = jnp.concatenate(ranks, axis=1)
    n_pair = jnp.broadcast_to(carry, (n_exp, lanes))

    exp_id = lax.broadcasted_iota(jnp.int32, (n_exp, lanes), 0)
    match = [[(exp_id == table[d, s]).astype(f32) for s in range(n_slot)] for d in peers]
    copies = sum(sum(row) for row in match)
    per_copy = 1.0 / copies
    hot = (copies == 4.0).astype(f32)
    own = sum(match[0])
    own_slot = sum(s * match[0][s] for s in range(n_slot))
    seen = jnp.zeros((n_exp, lanes), f32)
    start_out = [jnp.zeros((n_exp, lanes), f32) for _ in range(MAX_COPIES)]
    start_back = [jnp.zeros((n_exp, lanes), f32) for _ in range(MAX_COPIES)]
    stream_counts, over_out, over_back = [], [], []
    for r in range(len(peers)):
        seens, counts = [], []
        peer_hot = jnp.zeros((1, lanes), f32)
        for s in range(n_slot):
            here = match[r][s]
            seens.append(seen)
            rows = jnp.floor((n_pair - seen + copies - 0.5) * per_copy)
            counts.append(jnp.sum(here * (1.0 - own) * rows, axis=0, keepdims=True))
            peer_hot = peer_hot + s * jnp.sum(here * hot, axis=0, keepdims=True)
            seen = seen + here
        out_at, back_at, out_end, back_end = stream_starts(counts, peer_hot)
        if r == 0:
            hot_slot = peer_hot
        if r >= 2:
            stream_counts.append(counts)
            over_out.append(jnp.maximum(out_end - DIRECT, 0.0))
            over_back.append(jnp.maximum(back_end - DIRECT, 0.0))
        for s in range(n_slot):
            local = LOCAL_BASE + SLOT_ROWS * own_slot + SEG * r
            if r == 0:
                code_out = code_back = local
            elif r == 1:
                seg = s - (peer_hot < s).astype(f32)
                code_out = code_back = jnp.where(own > 0, local, STREAM_AT[1] + SEG * seg)
            else:
                code_out = jnp.where(own > 0, local, RAW_AT[r] + out_at[s])
                code_back = jnp.where(own > 0, local, RAW_AT[r] + back_at[s])
            for c in range(MAX_COPIES):
                mine = (match[r][s] > 0) & (seens[s] == c)
                start_out[c] = jnp.where(mine, code_out, start_out[c])
                start_back[c] = jnp.where(mine, code_back, start_back[c])

    wide = lambda a: jnp.concatenate([a] * (n_tok // lanes), axis=1)
    row = jnp.floor((rank + 0.5) * wide(per_copy))
    which = rank - row * wide(copies)
    codes = []
    for starts, over in ((start_out, over_out), (start_back, over_back)):
        start = wide(starts[3])
        for c in range(MAX_COPIES - 1):
            start = jnp.where(which == c, wide(starts[c]), start)
        raw = jnp.sum(onehot * (start + row), axis=0, keepdims=True)
        code = raw
        for r, first in ((2, 0.0), (3, over[0][:, :1])):
            at = raw - RAW_AT[r]
            code = jnp.where(at >= 0, jnp.where(at < DIRECT, STREAM_AT[r] + at, SHARED_AT + first + (at - DIRECT)), code)
        codes.append(code.astype(jnp.int32))
    over = jnp.maximum(over_out[0] + over_out[1], over_back[0] + over_back[1])
    fits = jnp.max(own * hot, axis=0, keepdims=True) * (over <= SHARED).astype(f32)
    zero = jnp.zeros((1, lanes), f32)
    tables = [jnp.concatenate(stream_counts[0] + [zero] * (8 - n_slot), axis=0),
              jnp.concatenate(stream_counts[1] + [over_out[0], over_back[0]] + [zero] * (6 - n_slot), axis=0)]
    return codes, hot_slot, tables, fits


def layer_kernel(slot_expert, topk_idx, topk_w, tokens, w_up, w_down, out, last_rows, last_mask, last_gate, found, table, idx_row, gate_row, tok_buf, up_buf, down_buf, send_core, recv_core, send_chip, send_shared, recv_chip, acc, rows_buf, back_core, back_chip, back_shared, swap_out, swap_in, early, mixed, mask_buf, gate_buf, code_row, back_row, code_col, gate_col, counts_out, counts_in, flags, t_sem, w_sem, ds_sem, dr_sem, bs_sem, br_sem, o_sem, cs_sem, cr_sem, fs_sem, fr_sem, xs_sem, xr_sem):
    f32, bf16 = jnp.float32, jnp.bfloat16
    n_tok, d_model = tok_buf.shape
    n_slot = w_up.shape[0]
    d_ff = w_up.shape[2]
    me = lax.axis_index('ep')
    group = lax.axis_index('dp')
    chip, core = me // 2, me % 2
    peers = [me, 2 * chip + (1 - core), 2 * (1 - chip) + core, 2 * (1 - chip) + (1 - core)]
    peer_ids = [None] + [{'ep': peers[r]} for r in (1, 2, 3)] + [{'dp': 1 - group}]

    barrier = pltpu.get_barrier_semaphore()
    for r in (1, 2, 3, 4):
        pl.semaphore_signal(barrier, inc=1, device_id=peer_ids[r], device_id_type=MESH)

    def weight_copies(s):
        b = s % N_WBUF
        return (pltpu.make_async_copy(w_up.at[s], up_buf.at[b], w_sem.at[s, 0]),
                pltpu.make_async_copy(w_down.at[s], down_buf.at[b], w_sem.at[s, 1]))

    small_copies = [pltpu.make_async_copy(slot_expert, table, t_sem.at[0]),
                    pltpu.make_async_copy(topk_idx, idx_row, t_sem.at[1]),
                    pltpu.make_async_copy(topk_w, gate_row, t_sem.at[2])]
    token_copy = pltpu.make_async_copy(tokens, tok_buf, t_sem.at[3])
    for copy in small_copies:
        copy.start()
    token_copy.start()
    for copy in small_copies:
        copy.wait()
    (code_out, code_back), hot_slot, count_tables, fits = route(idx_row[...], table, peers, 16, n_slot)
    code_row[...] = jnp.broadcast_to(code_out, code_row.shape)
    back_row[...] = jnp.broadcast_to(code_back, back_row.shape)
    hot_slot = hot_slot[:, :1]
    for r in (2, 3):
        counts_out[r - 2] = count_tables[r - 2]
    flags[0] = jnp.broadcast_to(fits, (8, 128))

    def pick(ids):
        mask = (ids == code_row[0:1, :]).astype(f32).astype(bf16)
        return jnp.dot(mask, tok_buf[...], preferred_element_type=f32).astype(bf16)

    def ids_from(first, rows):
        return lax.broadcasted_iota(jnp.int32, (rows, n_tok), 0) + first

    def dispatch_copy(k, r):
        to = r
        if r == 1:
            rows = pl.ds(k * SEG, SEG)
            src, dst = send_core.at[rows], recv_core.at[rows]
        elif k < N_SEG - 1:
            rows = pl.ds(SEND_AT[k], SEND_AT[k + 1] - SEND_AT[k])
            src, dst = send_chip.at[r - 2, rows], recv_chip.at[r - 2, rows]
        elif r == 2:
            src, dst = send_shared, recv_chip.at[0, pl.ds(DIRECT, SHARED)]
        else:
            to = 1
            src, dst = recv_chip.at[0, pl.ds(DIRECT, SHARED)], recv_chip.at[1, pl.ds(DIRECT, SHARED)]
        return pltpu.make_async_remote_copy(
            src_ref=src, dst_ref=dst, send_sem=ds_sem.at[k, r - 1], recv_sem=dr_sem.at[k, r - 1],
            device_id=peer_ids[to], device_id_type=MESH)

    def back_copy(k, r):
        size = BACK_AT[k + 1] - BACK_AT[k]
        if r == 1:
            src, to_early, to_last = back_core.at[pl.ds(k * SEG, SEG)], pl.ds(k * SEG, SEG), pl.ds(0, SEG)
        else:
            src = back_chip.at[r - 2, pl.ds(BACK_AT[k], size)]
            to_early = pl.ds(3 * SEG + (r - 2) * BACK_AT[3] + BACK_AT[k], size)
            to_last = pl.ds(SEG + (r - 2) * size, size)
        return pltpu.make_async_remote_copy(
            src_ref=src, dst_ref=early.at[to_early] if k < N_SEG - 1 else last_rows.at[to_last],
            send_sem=bs_sem.at[k, r - 1], recv_sem=br_sem.at[k, r - 1],
            device_id=peer_ids[r], device_id_type=MESH)

    last_size = BACK_AT[N_SEG] - BACK_AT[N_SEG - 1]

    def shared_copy(r):
        if r == 1:
            src, dst = swap_out, swap_in
        else:
            src, dst = back_shared, last_rows.at[pl.ds(SEG + 2 * last_size, SHARED)]
        return pltpu.make_async_remote_copy(
            src_ref=src, dst_ref=dst, send_sem=xs_sem.at[r - 1], recv_sem=xr_sem.at[r - 1],
            device_id=peer_ids[r], device_id_type=MESH)

    def counts_copy(r):
        return pltpu.make_async_remote_copy(
            src_ref=counts_out.at[r - 2], dst_ref=counts_in.at[r - 2], send_sem=cs_sem.at[r - 2], recv_sem=cr_sem.at[r - 2],
            device_id=peer_ids[r], device_id_type=MESH)

    def flag_copy(r):
        src, dst = (0, 1) if r == 4 else (2, 2 + r)
        return pltpu.make_async_remote_copy(
            src_ref=flags.at[src], dst_ref=flags.at[dst], send_sem=fs_sem.at[r - 1], recv_sem=fr_sem.at[r - 1],
            device_id=peer_ids[r], device_id_type=MESH)

    token_copy.wait()
    for s in range(N_WBUF):
        for copy in weight_copies(s):
            copy.start()
    for k in range(N_SEG):
        if k < N_SEG - 1:
            size = SEND_AT[k + 1] - SEND_AT[k]
            ids = [ids_from(STREAM_AT[2] + SEND_AT[k], size), ids_from(STREAM_AT[3] + SEND_AT[k], size), ids_from(k * SEG, SEG)]
            picked = pick(jnp.concatenate(ids, axis=0))
            send_chip[0, SEND_AT[k]:SEND_AT[k + 1], :] = picked[:size]
            send_chip[1, SEND_AT[k]:SEND_AT[k + 1], :] = picked[size:2 * size]
        else:
            picked = pick(jnp.concatenate([ids_from(SHARED_AT, SHARED), ids_from(k * SEG, SEG)], axis=0))
            send_shared[...] = picked[:SHARED]
        send_core[k * SEG:(k + 1) * SEG, :] = picked[-SEG:]
        if k == 0:
            pl.semaphore_wait(barrier, 4)
            for r in (2, 3):
                counts_copy(r).start()
        for r in (2, 3, 1) if k < N_SEG - 1 else (2, 1):
            dispatch_copy(k, r).start()
    flag_copy(4).start()

    for s in range(n_slot):
        rows_buf[s * SLOT_ROWS:(s + 1) * SLOT_ROWS, :] = pick(ids_from(LOCAL_BASE + s * SLOT_ROWS, SLOT_ROWS))
    code_col[...] = jnp.transpose(jnp.broadcast_to(code_back, (128, n_tok)))
    gate_col[...] = jnp.transpose(jnp.broadcast_to(gate_row[...], (128, n_tok)))
    n_early = 3 * SEG + 2 * BACK_AT[3]
    early[n_early:, :] = jnp.zeros((EARLY_ROWS - n_early, d_model), bf16)
    rows_buf[n_slot * SLOT_ROWS:, :] = jnp.zeros((LOCAL_ROWS - n_slot * SLOT_ROWS, d_model), bf16)

    def piecewise(i, pieces):
        ids, at = jnp.full_like(i, -1), sum(size for _, size in pieces)
        for first, size in reversed(pieces):
            ids = jnp.where(i < at, i + (first - at + size), ids)
            at -= size
        return ids

    last_ids = lambda i: piecewise(i, [(STREAM_AT[1] + 3 * SEG, SEG), (STREAM_AT[2] + BACK_AT[3], last_size),
                                       (STREAM_AT[3] + BACK_AT[3], last_size), (SHARED_AT, SHARED)])
    early_ids = lambda i: piecewise(i, [(STREAM_AT[1], 3 * SEG), (STREAM_AT[2], BACK_AT[3]), (STREAM_AT[3], BACK_AT[3])])
    n_last = SEG + 2 * last_size + SHARED

    ids = last_ids(lax.broadcasted_iota(jnp.int32, (n_last, n_tok), 0))
    gates = jnp.sum(jnp.where(ids == back_row[0:1, :], gate_row[...], 0.0), axis=1, keepdims=True)
    gate_buf[...] = jnp.broadcast_to(gates, gate_buf.shape)
    lane = lax.broadcasted_iota(jnp.int32, (n_tok, 128), 1)
    for j in range(LAST_ROWS // 128):
        mask_buf[:, j * 128:(j + 1) * 128] = (code_col[...] == last_ids(lane + 128 * j)).astype(f32).astype(bf16)
    side_copies = [pltpu.make_async_copy(mask_buf, last_mask, t_sem.at[4]),
                   pltpu.make_async_copy(gate_buf, last_gate, t_sem.at[5])]
    for copy in side_copies:
        copy.start()
    flag_copy(4).wait_recv()
    flags[2] = jnp.minimum(flags[0], flags[1])
    for r in (1, 2, 3):
        flag_copy(r).start()
    for r in (2, 3):
        counts_copy(r).wait_recv()
    in_counts = [[counts_in[j, s:s + 1, :1] for s in range(n_slot)] for j in range(2)]
    in_first = [[counts_in[j, n_slot + d:n_slot + d + 1, :1] for d in range(2)] for j in range(2)]
    in_starts = [stream_starts(counts, hot_slot) for counts in in_counts]
    as_int = lambda a: a.astype(jnp.int32)

    def returned(r, first, size, slots, shift):
        slots = list(slots)
        i = lax.broadcasted_iota(jnp.int32, (size, SEG * len(slots)), 0)
        j = lax.broadcasted_iota(jnp.int32, (size, SEG * len(slots)), 1)
        mask = jnp.zeros(i.shape, f32)
        for n, q in enumerate(slots):
            row = j - n * SEG
            at = row + as_int(in_starts[r - 2][1][q])
            fit = (at + shift == i + first) & (at >= first) & (row >= 0) & (row < as_int(in_counts[r - 2][q]))
            mask = jnp.where(fit, 1.0, mask)
        done = jnp.concatenate([rows_buf[q * SLOT_ROWS + r * SEG:q * SLOT_ROWS + (r + 1) * SEG, :] for q in slots], axis=0)
        return jnp.dot(mask.astype(bf16), done, preferred_element_type=f32).astype(bf16)

    half = SLOT_ROWS // 2

    def experts(s, first, size, width):
        b = s % N_WBUF
        rows = pl.ds(pl.multiple_of(s * SLOT_ROWS + first, half), size)

        def ff_step(i, carry):
            cols = pl.ds(pl.multiple_of(i * width, width), width)
            pre = jnp.dot(rows_buf[rows, :], up_buf[b, :, cols], preferred_element_type=f32)
            hidden = jax.nn.gelu(pre, approximate=True).astype(bf16)
            acc[:size, :] += jnp.dot(hidden, down_buf[b, cols, :], preferred_element_type=f32)
            return carry

        acc[:size, :] = jnp.zeros((size, d_model), f32)
        lax.fori_loop(0, d_ff // width, ff_step, 0)
        rows_buf[rows, :] = acc[:size, :].astype(bf16)

    def near_in(s):
        lo = s * SLOT_ROWS + SEG
        if s < N_SEG:
            dispatch_copy(s, 1).wait_recv()
        mixed_in = rows_buf[lo:lo + SEG, :].astype(f32)
        if s < N_SEG:
            mixed_in = mixed_in + recv_core[s * SEG:(s + 1) * SEG, :].astype(f32) * (hot_slot > s).astype(f32)
        if s > 0:
            mixed_in = mixed_in + recv_core[(s - 1) * SEG:s * SEG, :].astype(f32) * (hot_slot < s).astype(f32)
        rows_buf[lo:lo + SEG, :] = mixed_in.astype(bf16)

    def near_out(s):
        lo = s * SLOT_ROWS + SEG
        if s > 0:
            k = s - 1
            prev = rows_buf[lo - SLOT_ROWS:lo - SLOT_ROWS + SEG, :].astype(f32)
            last = rows_buf[lo:lo + SEG, :].astype(f32)
            back = prev * (hot_slot > k).astype(f32) + last * (hot_slot <= k).astype(f32)
            back_core[k * SEG:(k + 1) * SEG, :] = back.astype(bf16)
            back_copy(k, 1).start()

    def far_in(s):
        if s < N_SEG:
            for r in (2, 3) if s < N_SEG - 1 else (3,):
                dispatch_copy(s, r).wait_recv()
        come = SEND_AT[s + 1] if s < N_SEG - 1 else DIRECT + SHARED
        i = lax.broadcasted_iota(jnp.int32, (SEG, come), 0)
        j = lax.broadcasted_iota(jnp.int32, (SEG, come), 1)
        for r in (2, 3):
            at = i + as_int(in_starts[r - 2][0][s])
            if s >= N_SEG - 1:
                at = jnp.where(at < DIRECT, at, at + as_int(in_first[r - 2][0]))
            mask = (j == at) & (i < as_int(in_counts[r - 2][s]))
            came = jnp.dot(mask.astype(f32).astype(bf16), recv_chip[r - 2, :come, :], preferred_element_type=f32)
            rows = slice(s * SLOT_ROWS + r * SEG, s * SLOT_ROWS + (r + 1) * SEG)
            rows_buf[rows, :] = (rows_buf[rows, :].astype(f32) + came).astype(bf16)

    def far_out(s):
        if s > 0:
            k = s - 1
            if k == N_SEG - 1:
                swap_out[...] = returned(3, DIRECT, SHARED, (s - 1, s), as_int(in_first[1][1]))
                shared_copy(1).start()
            for r in (2, 3):
                back_chip[r - 2, BACK_AT[k]:BACK_AT[k + 1], :] = returned(r, BACK_AT[k], BACK_AT[k + 1] - BACK_AT[k], range(max(k - 2, 0), s + 1), 0)
                back_copy(k, r).start()
            if k == N_SEG - 1:
                mine = returned(2, DIRECT, SHARED, (s - 1, s), as_int(in_first[0][1]))
                shared_copy(1).wait_recv()
                back_shared[...] = (mine.astype(f32) + swap_in[...].astype(f32)).astype(bf16)
                shared_copy(2).start()

    def weights_in(s):
        for copy in weight_copies(s):
            copy.wait()

    def prepare(s):
        near_in(s)
        far_in(s)
        weights_in(s)

    def finish(s):
        if s == N_SEG - 2:
            dispatch_copy(N_SEG - 1, 2).wait_recv()
            dispatch_copy(N_SEG - 1, 3).start()
        far_out(s)
        near_out(s)

    near_in(0)
    weights_in(0)
    experts(0, 0, half, FF_TILE)
    far_in(0)
    experts(0, half, half, FF_TILE)
    for copy in weight_copies(N_WBUF):
        copy.start()
    inner = range(1, n_slot)

    def step(t, carry):
        for q in inner:
            pl.when(t == q)(functools.partial(prepare, q))
        experts(t, 0, SLOT_ROWS, d_ff)
        for q in inner:
            pl.when(t == q)(functools.partial(finish, q))
        return carry

    lax.fori_loop(1, n_slot, step, 0)
    tile = 256
    n_tile = n_tok // tile

    def out_copy(i):
        at = pl.ds(pl.multiple_of(i * tile, tile), tile)
        return pltpu.make_async_copy(mixed.at[at], out.at[at], o_sem.at[i])

    def combine(ids_of, rows, source, final):
        def body(i, carry):
            at = pl.ds(pl.multiple_of(i * tile, tile), tile)
            mine = code_col[at, :]
            lane = lax.broadcasted_iota(jnp.int32, (tile, 128), 1)
            mask = jnp.concatenate([(mine == ids_of(lane + 128 * j)).astype(f32).astype(bf16) for j in range(rows // 128)], axis=1)
            part = jnp.dot(mask, source[...], preferred_element_type=f32)
            if final:
                part = part + mixed[at, :].astype(f32)
                part = part * jnp.concatenate([gate_col[at, :]] * (d_model // 128), axis=1)
            mixed[at, :] = part.astype(bf16)
            if final:
                out_copy(i).start()
            return carry
        lax.fori_loop(0, n_tile, body, 0)

    combine(lambda i: LOCAL_BASE + i, LOCAL_ROWS, rows_buf, False)
    for r in (1, 2, 3):
        flag_copy(r).wait_recv()
    agreed = jnp.minimum(jnp.minimum(flags[2], flags[3]), jnp.minimum(flags[4], flags[5]))
    found[...] = agreed[0:1, :].astype(jnp.int32)
    for k in range(N_SEG):
        for r in (1, 2, 3):
            back_copy(k, r).wait_recv()
        if k == N_SEG - 1:
            shared_copy(2).wait_recv()
        if k == N_SEG - 2:
            combine(early_ids, EARLY_ROWS, early, True)
            for i in range(n_tile):
                out_copy(i).wait()
            for copy in side_copies:
                copy.wait()
    for r in (2, 3):
        counts_copy(r).wait_send()
    for r in (1, 2):
        shared_copy(r).wait_send()
    for r in (1, 2, 3, 4):
        flag_copy(r).wait_send()
    for k in range(N_SEG):
        for r in (1, 2, 3):
            dispatch_copy(k, r).wait_send()
            back_copy(k, r).wait_send()


def last_kernel(part, rows, mask, gate, out):
    f32, bf16 = jnp.float32, jnp.bfloat16
    d_model = part.shape[1]
    gates = jnp.concatenate([gate[...]] * (d_model // 128), axis=1)
    scaled = (rows[...].astype(f32) * gates).astype(bf16)
    scaled = jnp.concatenate([scaled, jnp.zeros((LAST_ROWS - scaled.shape[0], d_model), bf16)], axis=0)
    late = jnp.dot(mask[...], scaled, preferred_element_type=f32)
    out[...] = (late + part[...].astype(f32)).astype(bf16)


def add_last(part, rows, mask, gate):
    n_tok, d_model = part.shape
    tile = 512
    by_tile = lambda cols: pl.BlockSpec((tile, cols), lambda i: (i, 0))
    whole = lambda a: pl.BlockSpec(a.shape, lambda i: (0, 0))
    return pl.pallas_call(
        last_kernel,
        grid=(n_tok // tile,),
        out_shape=jax.ShapeDtypeStruct(part.shape, part.dtype),
        in_specs=[by_tile(d_model), whole(rows), by_tile(mask.shape[1]), whole(gate)],
        out_specs=by_tile(d_model),
    )(part, rows, mask, gate)


def fast_layer(tokens, topk_idx, topk_w, w_up, w_down, slot_expert):
    n_tok, d_model = tokens.shape
    n_slot, d_ff = w_up.shape[1], w_up.shape[3]
    vmem = pl.BlockSpec(memory_space=pltpu.VMEM)
    anym = pl.BlockSpec(memory_space=pl.ANY)
    bf16, f32 = jnp.bfloat16, jnp.float32
    shape = jax.ShapeDtypeStruct
    dma = pltpu.SemaphoreType.DMA
    return pl.pallas_call(
        layer_kernel,
        out_shape=(shape((n_tok, d_model), bf16), shape((3 * SEG, d_model), bf16), shape((n_tok, LAST_ROWS), bf16),
                   shape((3 * SEG, 128), f32), shape((1, 128), jnp.int32)),
        in_specs=[anym] * 6,
        out_specs=(anym, anym, anym, anym, vmem),
        scratch_shapes=[
            pltpu.SMEM(slot_expert.shape, jnp.int32),
            pltpu.VMEM((1, n_tok), jnp.int32),
            pltpu.VMEM((1, n_tok), f32),
            pltpu.VMEM((n_tok, d_model), bf16),
            pltpu.VMEM((N_WBUF, d_model, d_ff), bf16),
            pltpu.VMEM((N_WBUF, d_ff, d_model), bf16),
            pltpu.VMEM((N_SEG * SEG, d_model), bf16),
            pltpu.VMEM((N_SEG * SEG, d_model), bf16),
            pltpu.VMEM((2, DIRECT, d_model), bf16),
            pltpu.VMEM((SHARED, d_model), bf16),
            pltpu.VMEM((2, DIRECT + SHARED, d_model), bf16),
            pltpu.VMEM((SLOT_ROWS, d_model), f32),
            pltpu.VMEM((LOCAL_ROWS, d_model), bf16),
            pltpu.VMEM((N_SEG * SEG, d_model), bf16),
            pltpu.VMEM((2, DIRECT, d_model), bf16),
            pltpu.VMEM((SHARED, d_model), bf16),
            pltpu.VMEM((SHARED, d_model), bf16),
            pltpu.VMEM((SHARED, d_model), bf16),
            pltpu.VMEM((EARLY_ROWS, d_model), bf16),
            pltpu.VMEM((n_tok, d_model), bf16),
            pltpu.VMEM((n_tok, LAST_ROWS), bf16),
            pltpu.VMEM((3 * SEG, 128), f32),
            pltpu.VMEM((8, n_tok), jnp.int32),
            pltpu.VMEM((8, n_tok), jnp.int32),
            pltpu.VMEM((n_tok, 128), jnp.int32),
            pltpu.VMEM((n_tok, 128), f32),
            pltpu.VMEM((2, 8, 128), f32),
            pltpu.VMEM((2, 8, 128), f32),
            pltpu.VMEM((6, 8, 128), f32),
            dma((6,)), dma((n_slot, 2)),
            dma((N_SEG, 3)), dma((N_SEG, 3)), dma((N_SEG, 3)), dma((N_SEG, 3)),
            dma((n_tok // 256,)), dma((2,)), dma((2,)), dma((4,)), dma((4,)), dma((2,)), dma((2,)),
        ],
        compiler_params=pltpu.CompilerParams(collective_id=0, has_side_effects=True, vmem_limit_bytes=60 * 1024 * 1024),
    )(slot_expert, topk_idx.reshape(1, n_tok), topk_w.reshape(1, n_tok), tokens, w_up[0], w_down[0])


def solution(mesh):
    def group_layer(tokens, topk_idx, topk_w, w_up, w_down, slot_expert):
        *parts, found = fast_layer(tokens, topk_idx, topk_w, w_up, w_down, slot_expert)
        args = (*parts, tokens, topk_idx, topk_w, w_up, w_down, slot_expert)
        return lax.cond(found[0, 0] == 1, lambda *a: add_last(*a[:4]), lambda *a: general_layer(*a[4:]), *args)

    row_spec = P(('dp', 'ep'), None)
    weight_spec = P('ep', None, None, None)
    return jax.shard_map(group_layer, mesh=mesh, in_specs=(row_spec, row_spec, row_spec, weight_spec, weight_spec, P(None, None)), out_specs=row_spec, check_vma=False)
```
